128 devices in a mesh: seq: 64 (over z_hi, y, x, core), head: 2 (over z_lo).
Axes of the slice: x: 4, y: 4, z: 4 (z_hi: 2, z_lo: 2; z = z_hi * 2 + z_lo), core: 2. Of those that a mesh axis runs over, the one named last changes fastest.
Arguments:
- queries: bfloat16 [12288, 4096], P('seq', 'head'), may hold values from -6 to 6
- key_states: bfloat16 [12288, 512], P('seq', 'head'), may hold values from -6 to 6
- value_states: bfloat16 [12288, 512], P('seq', 'head'), may hold values from -6 to 6
- positions: int32 [12288], P('seq'), may hold values from 0 to 12287, as said below
- out_weight: bfloat16 [4096, 4096], P('head'), may hold values from -0.125 to 0.125
Outputs:
- mixed: bfloat16 [12288, 4096], P('seq', 'head')
The draws below stay inside these ranges and needn't reach their ends.
Inputs may be any that keep to these rules, and one draw needn't show every extreme that they name: The sequence is cut into 128 blocks of 96 consecutive positions. The 192 rows of one index of seq hold two whole blocks in order, block b and block 127 - b for some b below 64, each block's positions ascending; every position appears once.
All inputs are finite; a program needn't handle non-finite values.
Results may differ from the reference program's by a relative error of at most 0.0095.
Values may be sent and summed in bfloat16 or wider, within the bound.
No kernel may reach another device: no remote copies, remote signals or barrier semaphores. Data moves between devices by JAX's collectives and lax.ppermute only.
A program may use at most 128 MiB of HBM per device.

```python
import jax
import jax.numpy as jnp
from jax import lax

HQ = 32
KV = 4
HD = 128
DOUT = 4096
GROUP = 8
TOK_DEV = 192
BLK = 96
BLOCKS = 128
TOKENS = 12288
N_SEQ = 64


def layout(key):
    order = jax.random.permutation(jax.random.fold_in(key, 101), N_SEQ).astype(jnp.int32)
    rows_all = jnp.arange(TOKENS, dtype=jnp.int32)
    device = rows_all // TOK_DEV
    within = rows_all % TOK_DEV
    second = within // BLK
    offset = within % BLK
    first_block = order[device]
    chosen_block = jnp.where(second == 1, BLOCKS - 1 - first_block, first_block)
    return (chosen_block * BLK + offset).astype(jnp.int32)


def draw_queries(key, part):
    places = layout(key)
    base = jnp.clip(4.0 * jax.random.normal(jax.random.fold_in(key, 1), (TOKENS, KV, GROUP, HD), jnp.float32), -6.0, 6.0)
    return base.reshape(TOKENS, HQ * HD)[places].astype(jnp.bfloat16)


def draw_key_states(key, part):
    places = layout(key)
    base = jnp.clip(jax.random.normal(jax.random.fold_in(key, 2), (TOKENS, KV, HD), jnp.float32), -6.0, 6.0)
    return base.reshape(TOKENS, KV * HD)[places].astype(jnp.bfloat16)


def draw_positions(key, part):
    return layout(key)


def strengthened(entries, stream_key, source, target, parts, factor):
    owner, partner = [(jnp.arange(entries.shape[position]) // (entries.shape[position] // parts)).reshape([-1 if axis == position else 1 for axis in range(entries.ndim)]) for position in (source, target)]
    chosen = jax.random.permutation(stream_key, parts)[partner]
    strong = (owner == chosen) | (owner == (partner + parts // 2) % parts)
    return jnp.where(strong, factor * entries, entries)


def level_of(stream_key, extent, shards, least, largest):
    gain, own = 1.0, jax.random.fold_in(stream_key, 6)
    for position, shards_of in shards:
        steps = jnp.exp(jax.random.uniform(jax.random.fold_in(own, position), (shards_of,), jnp.float32, least / len(shards), largest / len(shards)))
        gain = gain * jnp.repeat(steps, extent[position] // shards_of).reshape([-1 if axis == position else 1 for axis in range(len(extent))])
    return gain


def bell_draw(key, shape, width, reach, split=(), kind=jnp.bfloat16):
    result = jax.random.normal(key, shape, jnp.float32) * width
    if len(split) > 0:
        result = level_of(key, shape, split, -0.22, 0.18) * result
    return jnp.clip(result, min=-reach, max=reach).astype(kind)


def noise_with(key, shape, deviation, most, shards, heavy, held_as=jnp.bfloat16):
    values = deviation * jax.random.normal(key, shape, jnp.float32)
    if shards:
        values = values * level_of(key, shape, shards, -0.22, 0.18)
    return jnp.clip(strengthened(values, jax.random.fold_in(key, 3), *heavy), -most, most).astype(held_as)


def setup_inputs(seed: int = 0) -> dict:
    key_list = jax.random.split(jax.random.key(seed), 6)
    queries = draw_queries(jax.random.fold_in(key_list[5], 71), 0)
    key_states = draw_key_states(jax.random.fold_in(key_list[5], 71), 0)
    value_states = bell_draw(key_list[2], (TOKENS, KV * HD), 1.0, 6.0, ((0, 64), (1, 2)))
    positions = draw_positions(jax.random.fold_in(key_list[5], 71), 0)
    out_weight = noise_with(key_list[4], (HQ * HD, DOUT), (HQ * HD) ** -0.5, 0.125, ((0, 2),), (0, 1, 2, 2.0))
    return {"queries": queries, "key_states": key_states, "value_states": value_states, "positions": positions, "out_weight": out_weight}


def reference(queries, key_states, value_states, positions, out_weight):
    score_scale = HD ** -0.5
    query_all = queries.astype(jnp.float32).reshape(TOKENS // TOK_DEV, TOK_DEV, KV, GROUP, HD)
    key_heads = key_states.astype(jnp.float32).reshape(TOKENS, KV, HD).transpose(1, 0, 2)
    value_heads = value_states.astype(jnp.float32).reshape(TOKENS, KV, HD).transpose(1, 0, 2)
    place_blocks = positions.reshape(TOKENS // TOK_DEV, TOK_DEV)

    def per_block(query_pair):
        query_block, query_place = query_pair
        visible = positions[None, None, :] <= query_place[None, :, None]

        def per_head(head_items):
            query_head, key_head, value_head = head_items
            scores = jnp.einsum("tgd,kd->gtk", query_head, key_head) * score_scale
            row_peak = jnp.max(jnp.where(visible, scores, -jnp.inf), axis=-1, keepdims=True)
            weights = jnp.where(visible, jnp.exp(scores - row_peak), 0.0)
            row_total = jnp.sum(weights, axis=-1, keepdims=True)
            rounded = lax.optimization_barrier(weights.astype(jnp.bfloat16)).astype(jnp.float32)
            return jnp.einsum("gtk,kd->gtd", rounded, value_head) / row_total

        heads_out = lax.map(per_head, (query_block.transpose(1, 0, 2, 3), key_heads, value_heads))
        return heads_out.transpose(2, 0, 1, 3).reshape(TOK_DEV, HQ * HD).astype(jnp.bfloat16)

    attended = lax.map(per_block, (query_all, place_blocks)).reshape(TOKENS, HQ * HD)
    return jnp.dot(attended, out_weight, preferred_element_type=jnp.float32).astype(jnp.bfloat16)
```

```python
import functools

import jax
import jax.numpy as jnp
import numpy as np
from jax import lax
from jax.experimental import pallas as pl
from jax.experimental.pallas import tpu as pltpu
from jax.sharding import Mesh, PartitionSpec as P

HD = 128
GROUP = 8
BLK = 96
ROWS = 200
QW = GROUP * BLK
SCALE = 1.4426950408889634 * HD**-0.5
LOWEST = -1e30


def shifted(array, axis, by):
    size = lax.axis_size(axis)
    return lax.ppermute(array, axis, [(i, (i + by) % size) for i in range(size)])


def fold(scores, vt, cols, m_ref, l_ref, o_ref):
    old = m_ref[:, cols]
    new = jnp.maximum(old, jnp.max(scores, axis=0, keepdims=True) * SCALE)
    weights = jnp.exp2(scores * SCALE - new)
    factor = jnp.exp2(old - new)
    m_ref[:, cols] = new
    l_ref[:, cols] = l_ref[:, cols] * factor + jnp.sum(weights, axis=0, keepdims=True)
    o_ref[:, cols] = o_ref[:, cols] * factor + jnp.dot(
        vt, weights.astype(jnp.bfloat16), preferred_element_type=jnp.float32
    )


def attend_kernel(counts, first, last, *refs):
    number = len(counts)
    b_ref = refs[0]
    pieces = refs[1 : 1 + number]
    refs = refs[1 + number :]
    if first:
        q_ref = refs[0]
        qt_ref, m_ref, l_ref, o_ref = refs[1:5]
        refs = refs[5:]
    else:
        qt_ref, m_in, l_in, o_in = refs[:4]
        if last:
            att_ref, m_ref, l_ref, o_ref = refs[4:8]
            refs = refs[8:]
        else:
            m_ref, l_ref, o_ref = refs[4:7]
            refs = refs[7:]
    vp_ref, vs_ref, kp_ref, ks_ref, tag_ref = refs

    at = 0
    for piece, count in zip(pieces, counts):
        for i in range(count):
            base = i * ROWS
            tag_ref[at + i] = jnp.max(
                piece[base + 2 * BLK : base + 2 * BLK + 8, :HD].astype(jnp.float32)
            ).astype(jnp.int32)
            for half in range(2):
                rows = slice(base + half * BLK, base + half * BLK + BLK)
                ks_ref[2 * (at + i) + half] = piece[rows, :HD]
                vs_ref[2 * (at + i) + half] = piece[rows, HD:].T
        for i in range(0, count, 2):
            low = [piece[(i + k) * ROWS : (i + k) * ROWS + BLK, :] for k in range(2)]
            both = jnp.concatenate(low, axis=0)
            kp_ref[(at + i) // 2] = both[:, :HD]
            vp_ref[(at + i) // 2] = both[:, HD:].T
        at += count
    total = at

    if first:
        for s in range(2):
            for half in range(2):
                rows = slice(half * BLK, half * BLK + BLK)
                tall = jnp.concatenate(
                    [q_ref[s, rows, h * HD : (h + 1) * HD] for h in range(GROUP)], axis=0
                )
                start = ((1 - half) * 2 + s) * QW
                qt_ref[:, start : start + QW] = tall.T
        m_ref[...] = jnp.full(m_ref.shape, LOWEST, jnp.float32)
        l_ref[...] = jnp.zeros(l_ref.shape, jnp.float32)
        o_ref[...] = jnp.zeros(o_ref.shape, jnp.float32)
        token = lax.rem(lax.broadcasted_iota(jnp.int32, (1, QW), 1), BLK)
        seen = lax.broadcasted_iota(jnp.int32, (BLK, QW), 0) <= token
        for s in range(2):
            for half in range(2):
                start = ((1 - half) * 2 + s) * QW
                cols = slice(start, start + QW)
                scores = jnp.dot(
                    ks_ref[2 * s + half], qt_ref[:, cols], preferred_element_type=jnp.float32
                )
                fold(jnp.where(seen, scores, LOWEST), vs_ref[2 * s + half], cols, m_ref, l_ref, o_ref)
    else:
        m_ref[...] = m_in[...]
        l_ref[...] = l_in[...]
        o_ref[...] = o_in[...]

    pairs = total // 2

    def low_step(step, carry):
        tile = lax.rem(step, 2)
        pair = lax.div(step, 2)
        cols = pl.ds(pl.multiple_of(tile * QW, 128), QW)
        scores = jnp.dot(kp_ref[pair], qt_ref[:, cols], preferred_element_type=jnp.float32)
        fold(scores, vp_ref[pair], cols, m_ref, l_ref, o_ref)
        return carry

    lax.fori_loop(0, 2 * pairs, low_step, 0)

    def pick_step(step, carry):
        s = lax.rem(step, 2)
        index = lax.div(step, 2)
        if first:
            index = index + 2
        low = tag_ref[index] < b_ref[s]
        half = jnp.where(low, 0, 1)
        cols = pl.ds(pl.multiple_of(jnp.where(low, 2 * QW, 0) + s * QW, 128), QW)
        scores = jnp.dot(
            ks_ref[2 * index + half], qt_ref[:, cols], preferred_element_type=jnp.float32
        )
        fold(scores, vs_ref[2 * index + half], cols, m_ref, l_ref, o_ref)
        return carry

    if first:
        for s in range(2):
            index = 1 - s
            low = tag_ref[index] < b_ref[s]
            half = jnp.where(low, 0, 1)
            cols = pl.ds(pl.multiple_of(jnp.where(low, 2 * QW, 0) + s * QW, 128), QW)
            scores = jnp.dot(
                ks_ref[2 * index + half], qt_ref[:, cols], preferred_element_type=jnp.float32
            )
            fold(scores, vs_ref[2 * index + half], cols, m_ref, l_ref, o_ref)
        lax.fori_loop(0, 2 * (total - 2), pick_step, 0)
    else:
        lax.fori_loop(0, 2 * total, pick_step, 0)

    if last:
        for s in range(2):
            for half in range(2):
                start = ((1 - half) * 2 + s) * QW
                cols = slice(start, start + QW)
                done = (o_ref[:, cols] / l_ref[:, cols]).T
                for h in range(GROUP):
                    att_ref[s, half * BLK : (half + 1) * BLK, h * HD : (h + 1) * HD] = done[
                        h * BLK : (h + 1) * BLK
                    ].astype(jnp.bfloat16)


def attend(b_both, pieces, state, first=False, last=False):
    counts = tuple(p.shape[0] // ROWS for p in pieces)
    total = sum(counts)
    vmem = pl.BlockSpec(memory_space=pltpu.VMEM)
    smem = pl.BlockSpec(memory_space=pltpu.SMEM)
    width = 4 * QW
    kept = [
        jax.ShapeDtypeStruct((1, width), jnp.float32),
        jax.ShapeDtypeStruct((1, width), jnp.float32),
        jax.ShapeDtypeStruct((HD, width), jnp.float32),
    ]
    if first:
        outs = [jax.ShapeDtypeStruct((HD, width), jnp.bfloat16)] + kept
        aliases = {}
    elif last:
        outs = [jax.ShapeDtypeStruct((2, 2 * BLK, GROUP * HD), jnp.bfloat16)] + kept
        aliases = {2 + len(pieces) + i: 1 + i for i in range(3)}
    else:
        outs = kept
        aliases = {2 + len(pieces) + i: i for i in range(3)}
    cells = total * 2 * BLK * BLK * 2 * GROUP
    return pl.pallas_call(
        functools.partial(attend_kernel, counts, first, last),
        out_shape=outs,
        in_specs=[smem] + [vmem] * (len(pieces) + len(state)),
        out_specs=[vmem] * len(outs),
        input_output_aliases=aliases,
        scratch_shapes=[
            pltpu.VMEM((total // 2, HD, 2 * BLK), jnp.bfloat16),
            pltpu.VMEM((2 * total, HD, BLK), jnp.bfloat16),
            pltpu.VMEM((total // 2, 2 * BLK, HD), jnp.bfloat16),
            pltpu.VMEM((2 * total, BLK, HD), jnp.bfloat16),
            pltpu.SMEM((total,), jnp.int32),
        ],
        cost_estimate=pl.CostEstimate(
            flops=4 * HD * cells, transcendentals=cells, bytes_accessed=total * ROWS * 512
        ),
    )(b_both, *pieces, *state)


def ring(array, axis):
    half = array.shape[0] // 2
    left = shifted(array, axis, 1)
    right = shifted(array, axis, -1)
    far_left = shifted(left[:half], axis, 1)
    far_right = shifted(right[half:], axis, -1)
    return [left, right], [far_left, far_right]


def shards(queries, key_states, value_states, positions, out_weight):
    core = lax.axis_index("core")
    first_core = core == 0
    block = lax.div(positions[0], BLK)

    def packed(low):
        cut = slice(0, HD) if low else slice(HD, 2 * HD)
        rows = jnp.concatenate([key_states[:, cut], value_states[:, cut]], axis=1)
        return jnp.concatenate(
            [rows, jnp.broadcast_to(block.astype(jnp.bfloat16), (ROWS - 2 * BLK, 2 * HD))], axis=0
        )

    low, high = packed(True), packed(False)
    given = shifted(jnp.where(first_core, high, low), "core", 1)
    own = jnp.where(first_core, low, high)
    both = jnp.concatenate([own, given], axis=0)
    b_both = jnp.stack([block, given[2 * BLK, 0].astype(jnp.int32)])
    width = GROUP * HD
    q_low, q_high = queries[:, :width], queries[:, width:]
    q_given = shifted(jnp.where(first_core, q_high, q_low), "core", 1)
    q_both = jnp.stack([jnp.where(first_core, q_low, q_high), q_given])

    beyond = shifted(both, "z", 1)
    near_a, far_a = ring(both, "x")
    near_b, far_b = ring(beyond, "y")
    state = attend(b_both, [both, beyond], [q_both], first=True)
    qt, state = state[0], state[1:]
    state = attend(b_both, near_a + near_b + [jnp.concatenate(far_a), jnp.concatenate(far_b)], [qt, *state])
    all_a = jnp.concatenate([both] + near_a + far_a, axis=0)
    all_b = jnp.concatenate([beyond] + near_b + far_b, axis=0)
    near_a, far_a = ring(all_a, "y")
    near_b, far_b = ring(all_b, "x")
    state = attend(b_both, near_a + near_b, [qt, *state])
    done = attend(b_both, far_a + far_b, [qt, *state], last=True)[0]

    returned = shifted(done[1], "core", 1)
    attended = jnp.where(
        first_core,
        jnp.concatenate([done[0], returned], axis=1),
        jnp.concatenate([returned, done[0]], axis=1),
    )
    partial_sum = jnp.dot(attended, out_weight, preferred_element_type=jnp.float32)
    half = partial_sum.shape[1] // 2
    here = lax.axis_index("head") == 0
    kept = jnp.where(here, partial_sum[:, :half], partial_sum[:, half:])
    sent = jnp.where(here, partial_sum[:, half:], partial_sum[:, :half]).astype(jnp.bfloat16)
    return (kept + shifted(sent, "head", 1).astype(jnp.float32)).astype(jnp.bfloat16)


def solution(mesh):
    split = Mesh(mesh.devices.reshape(2, 4, 4, 2, 2), ("z", "y", "x", "core", "head"))
    seq = ("z", "y", "x", "core")
    in_specs = (P(seq, "head"), P(seq, "head"), P(seq, "head"), P(seq), P("head", None))
    return jax.shard_map(
        shards, mesh=split, in_specs=in_specs, out_specs=P(seq, "head"), check_vma=False
    )
```

```python
import functools

import jax
import jax.numpy as jnp
import numpy as np
from jax import lax
from jax.experimental import pallas as pl
from jax.experimental.pallas import tpu as pltpu
from jax.sharding import Mesh, PartitionSpec as P

HD = 128
GROUP = 8
BLK = 96
ROWS = 200
QW = GROUP * BLK
SCALE = 1.4426950408889634 * HD**-0.5
LOWEST = -1e30
VMEM_BYTES = 24 << 20


def shifted(array, axis, by):
    size = lax.axis_size(axis)
    return lax.ppermute(array, axis, [(i, (i + by) % size) for i in range(size)])


def fold(scores, vt, cols, m_ref, l_ref, o_ref):
    old = m_ref[:, cols]
    new = jnp.maximum(old, jnp.max(scores, axis=0, keepdims=True) * SCALE)
    weights = jnp.exp2(scores * SCALE - new)
    factor = jnp.exp2(old - new)
    m_ref[:, cols] = new
    l_ref[:, cols] = l_ref[:, cols] * factor + jnp.sum(weights, axis=0, keepdims=True)
    o_ref[:, cols] = o_ref[:, cols] * factor + jnp.dot(
        vt, weights.astype(jnp.bfloat16), preferred_element_type=jnp.float32
    )


def staged(number, tiles, qt_ref, m_ref, l_ref, o_ref, s_refs, p_refs, f_refs):
    def score(step, slot):
        for t, (keys, _, cols) in enumerate(tiles(step)):
            k = keys.shape[0]
            s_refs[slot][t * k : (t + 1) * k] = jnp.dot(
                keys, qt_ref[:, cols], preferred_element_type=jnp.float32
            )

    def weigh(step, slot):
        for t, (keys, _, cols) in enumerate(tiles(step)):
            k = keys.shape[0]
            scores = s_refs[slot][t * k : (t + 1) * k]
            old = m_ref[:, cols]
            new = jnp.maximum(old, jnp.max(scores, axis=0, keepdims=True) * SCALE)
            weights = jnp.exp2(scores * SCALE - new)
            factor = jnp.exp2(old - new)
            m_ref[:, cols] = new
            l_ref[:, cols] = l_ref[:, cols] * factor + jnp.sum(weights, axis=0, keepdims=True)
            f_refs[slot][t] = factor
            p_refs[slot][t * k : (t + 1) * k] = weights.astype(jnp.bfloat16)

    def add(step, slot):
        for t, (keys, vt, cols) in enumerate(tiles(step)):
            k = keys.shape[0]
            o_ref[:, cols] = o_ref[:, cols] * f_refs[slot][t] + jnp.dot(
                vt(), p_refs[slot][t * k : (t + 1) * k], preferred_element_type=jnp.float32
            )

    def turn(j, carry):
        i = 2 * j
        for slot in range(2):
            score(i + 2 + slot, slot)
            weigh(i + 1 + slot, 1 - slot)
            add(i + slot, slot)
        return carry

    score(0, 0)
    score(1, 1)
    weigh(0, 0)
    lax.fori_loop(0, number // 2 - 1, turn, 0)
    weigh(number - 1, 1)
    add(number - 2, 0)
    add(number - 1, 1)


def attend_kernel(counts, first, last, *refs):
    number = len(counts)
    pieces = refs[:number]
    refs = refs[number:]
    if first:
        q_refs = refs[:2]
        b_ref, qt_ref, m_ref, l_ref, o_ref = refs[2:7]
        refs = refs[7:]
    else:
        b_ref, qt_ref, m_in, l_in, o_in = refs[:5]
        if last:
            att_refs = refs[5:7]
            refs = refs[7:]
        else:
            refs = refs[5:]
        m_ref, l_ref, o_ref = refs[:3]
        refs = refs[3:]
    vp_ref, vs_ref, kp_ref, ks_ref, tag_ref = refs[:5]
    s_refs, p_refs, f_refs = refs[5:7], refs[7:9], refs[9:11]
    kept = (qt_ref, m_ref, l_ref, o_ref, s_refs, p_refs, f_refs)

    places = [(p, i * ROWS) for p, count in zip(pieces, counts) for i in range(count)]
    total = len(places)
    for i, (piece, base) in enumerate(places):
        tag_ref[i] = jnp.max(
            piece[base + 2 * BLK : base + 2 * BLK + 8, :HD].astype(jnp.float32)
        ).astype(jnp.int32)
        for half in range(2):
            rows = slice(base + half * BLK, base + half * BLK + BLK)
            ks_ref[2 * i + half] = piece[rows, :HD]
            vs_ref[2 * i + half] = piece[rows, HD:].T
    for i in range(0, total, 2):
        both = jnp.concatenate([p[at : at + BLK, :] for p, at in places[i : i + 2]], axis=0)
        kp_ref[i // 2] = both[:, :HD]
        vp_ref[i // 2] = both[:, HD:].T
    if first:
        for s in range(2):
            b_ref[s] = tag_ref[s]

    if first:
        for s in range(2):
            for half in range(2):
                rows = slice(half * BLK, half * BLK + BLK)
                tall = jnp.concatenate(
                    [q_refs[s][rows, h * HD : (h + 1) * HD] for h in range(GROUP)], axis=0
                )
                start = ((1 - half) * 2 + s) * QW
                qt_ref[:, start : start + QW] = tall.T
        m_ref[...] = jnp.full(m_ref.shape, LOWEST, jnp.float32)
        l_ref[...] = jnp.zeros(l_ref.shape, jnp.float32)
        o_ref[...] = jnp.zeros(o_ref.shape, jnp.float32)
        token = lax.rem(lax.broadcasted_iota(jnp.int32, (1, QW), 1), BLK)
        seen = lax.broadcasted_iota(jnp.int32, (BLK, QW), 0) <= token
        for s in range(2):
            for half in range(2):
                start = ((1 - half) * 2 + s) * QW
                cols = slice(start, start + QW)
                scores = jnp.dot(
                    ks_ref[2 * s + half], qt_ref[:, cols], preferred_element_type=jnp.float32
                )
                fold(jnp.where(seen, scores, LOWEST), vs_ref[2 * s + half], cols, m_ref, l_ref, o_ref)
    else:
        m_ref[...] = m_in[...]
        l_ref[...] = l_in[...]
        o_ref[...] = o_in[...]

    def low_tiles(step):
        pair, s = lax.div(step, 2), lax.rem(step, 2)
        cols = pl.ds(pl.multiple_of(s * QW, 128), QW)
        return [(kp_ref[pair], lambda: vp_ref[pair], cols)]

    staged(total, low_tiles, *kept)

    def picked(index, s):
        low = tag_ref[index] < b_ref[s]
        at = 2 * index + jnp.where(low, 0, 1)
        cols = pl.ds(pl.multiple_of(jnp.where(low, 2 * QW, 0) + s * QW, 128), QW)
        return (ks_ref[at], lambda: vs_ref[at], cols)

    if first:
        for s in range(2):
            keys, vt, cols = picked(1 - s, s)
            scores = jnp.dot(keys, qt_ref[:, cols], preferred_element_type=jnp.float32)
            fold(scores, vt(), cols, m_ref, l_ref, o_ref)
    skipped = 2 if first else 0
    staged(
        total - skipped, lambda step: [picked(step + skipped, s) for s in range(2)], *kept
    )

    if last:
        for s in range(2):
            for half in range(2):
                start = ((1 - half) * 2 + s) * QW
                cols = slice(start, start + QW)
                done = (o_ref[:, cols] / l_ref[:, cols]).T
                for h in range(GROUP):
                    att_refs[s][half * BLK : (half + 1) * BLK, h * HD : (h + 1) * HD] = done[
                        h * BLK : (h + 1) * BLK
                    ].astype(jnp.bfloat16)


def attend(pieces, state, first=False, last=False):
    counts = tuple(p.shape[0] // ROWS for p in pieces)
    total = sum(counts)
    vmem = pl.BlockSpec(memory_space=pltpu.VMEM)
    smem = pl.BlockSpec(memory_space=pltpu.SMEM)
    width = 4 * QW
    kept = [
        jax.ShapeDtypeStruct((1, width), jnp.float32),
        jax.ShapeDtypeStruct((1, width), jnp.float32),
        jax.ShapeDtypeStruct((HD, width), jnp.float32),
    ]
    aliases = {}
    in_specs = [vmem] * (len(pieces) + len(state))
    if first:
        outs = [
            jax.ShapeDtypeStruct((2,), jnp.int32),
            jax.ShapeDtypeStruct((HD, width), jnp.bfloat16),
        ] + kept
        out_specs = [smem] + [vmem] * 4
    else:
        outs = [jax.ShapeDtypeStruct((2 * BLK, GROUP * HD), jnp.bfloat16)] * (2 * last) + kept
        out_specs = [vmem] * len(outs)
        in_specs[len(pieces)] = smem
        aliases = {2 + len(pieces) + i: 2 * last + i for i in range(3)}
    cells = total * 2 * BLK * BLK * 2 * GROUP
    return pl.pallas_call(
        functools.partial(attend_kernel, counts, first, last),
        out_shape=outs,
        in_specs=in_specs,
        out_specs=out_specs,
        input_output_aliases=aliases,
        scratch_shapes=[
            pltpu.VMEM((total // 2, HD, 2 * BLK), jnp.bfloat16),
            pltpu.VMEM((2 * total, HD, BLK), jnp.bfloat16),
            pltpu.VMEM((total // 2, 2 * BLK, HD), jnp.bfloat16),
            pltpu.VMEM((2 * total, BLK, HD), jnp.bfloat16),
            pltpu.SMEM((total,), jnp.int32),
        ]
        + [pltpu.VMEM((2 * BLK, QW), jnp.float32)] * 2
        + [pltpu.VMEM((2 * BLK, QW), jnp.bfloat16)] * 2
        + [pltpu.VMEM((2, 1, QW), jnp.float32)] * 2,
        cost_estimate=pl.CostEstimate(
            flops=4 * HD * cells, transcendentals=cells, bytes_accessed=total * ROWS * 512
        ),
        compiler_params=pltpu.CompilerParams(vmem_limit_bytes=VMEM_BYTES),
    )(*pieces, *state)


def pack_kernel(core_ref, place_ref, k_ref, v_ref, q_ref, own_ref, sent_ref, q_own_ref, q_sent_ref):
    core = core_ref[0]
    tag = lax.div(place_ref[0], BLK).astype(jnp.float32)
    tags = jnp.full((ROWS - 2 * BLK, 2 * HD), tag, jnp.float32).astype(jnp.bfloat16)
    width = GROUP * HD
    for which, kv_ref, to_ref in ((core, own_ref, q_own_ref), (1 - core, sent_ref, q_sent_ref)):
        cols = pl.ds(pl.multiple_of(which * HD, HD), HD)
        kv_ref[: 2 * BLK, :HD] = k_ref[:, cols]
        kv_ref[: 2 * BLK, HD:] = v_ref[:, cols]
        kv_ref[2 * BLK :, :] = tags
        to_ref[...] = q_ref[:, pl.ds(pl.multiple_of(which * width, HD), width)]


def pack(core, positions, keys, values, queries):
    vmem = pl.BlockSpec(memory_space=pltpu.VMEM)
    smem = pl.BlockSpec(memory_space=pltpu.SMEM)
    kv = jax.ShapeDtypeStruct((ROWS, 2 * HD), jnp.bfloat16)
    q = jax.ShapeDtypeStruct((2 * BLK, GROUP * HD), jnp.bfloat16)
    return pl.pallas_call(
        pack_kernel,
        out_shape=[kv, kv, q, q],
        in_specs=[smem, smem, vmem, vmem, vmem],
        out_specs=[vmem] * 4,
        compiler_params=pltpu.CompilerParams(vmem_limit_bytes=VMEM_BYTES),
    )(core[None], positions, keys, values, queries)


def join_kernel(number, *refs):
    parts, whole, sems = refs[:number], refs[number], refs[number + 1]
    copies, at = [], 0
    for i, part in enumerate(parts):
        rows = part.shape[0]
        copies.append(pltpu.make_async_copy(part, whole.at[pl.ds(at, rows)], sems.at[i]))
        at += rows
    for copy in copies:
        copy.start()
    for copy in copies:
        copy.wait()


def joined(parts):
    rows = sum(p.shape[0] for p in parts)
    anywhere = pl.BlockSpec(memory_space=pl.ANY)
    return pl.pallas_call(
        functools.partial(join_kernel, len(parts)),
        out_shape=jax.ShapeDtypeStruct((rows, parts[0].shape[1]), parts[0].dtype),
        in_specs=[anywhere] * len(parts),
        out_specs=anywhere,
        scratch_shapes=[pltpu.SemaphoreType.DMA((len(parts),))],
        compiler_params=pltpu.CompilerParams(vmem_limit_bytes=VMEM_BYTES),
    )(*parts)


def near(array, axis):
    return [shifted(array, axis, 1), shifted(array, axis, -1)]


def far(pair, axis):
    half = pair[0].shape[0] // 2
    return [shifted(pair[0][:half], axis, 1), shifted(pair[1][half:], axis, -1)]


def after(pairs, token):
    *arrays, _ = lax.optimization_barrier((*pairs[0], *pairs[1], token))
    return arrays[:2], arrays[2:]


def shards(queries, key_states, value_states, positions, out_weight):
    core = lax.axis_index("core")
    own, sent, q_own, q_sent = pack(core, positions, key_states, value_states, queries)
    both = joined([own, shifted(sent, "core", 1)])
    q_given = shifted(q_sent, "core", 1)

    beyond = shifted(both, "z", 1)
    near_a = near(both, "x")
    near_b = near(beyond, "y")
    b_both, qt, *state = attend([both, beyond], [q_own, q_given], first=True)
    near_a, near_b = after((near_a, near_b), state[1])
    far_a, far_b = far(near_a, "x"), far(near_b, "y")
    pieces = near_a + near_b + far_a + far_b
    all_a = joined([both] + near_a + far_a)
    all_b = joined([beyond] + near_b + far_b)
    near_a, near_b = near(all_a, "y"), near(all_b, "x")
    state = attend(pieces, [b_both, qt, *state])
    near_a, near_b = after((near_a, near_b), state[1])
    far_a, far_b = far(near_a, "y"), far(near_b, "x")
    state = attend(near_a + near_b, [b_both, qt, *state])
    mine, returned = attend(far_a + far_b, [b_both, qt, *state], last=True)[:2]

    returned = shifted(returned, "core", 1)
    attended = jnp.where(
        core == 0,
        jnp.concatenate([mine, returned], axis=1),
        jnp.concatenate([returned, mine], axis=1),
    )
    partial_sum = jnp.dot(attended, out_weight, preferred_element_type=jnp.float32)
    half = partial_sum.shape[1] // 2
    here = lax.axis_index("head") == 0
    kept = jnp.where(here, partial_sum[:, :half], partial_sum[:, half:])
    sent = jnp.where(here, partial_sum[:, half:], partial_sum[:, :half]).astype(jnp.bfloat16)
    return (kept + shifted(sent, "head", 1).astype(jnp.float32)).astype(jnp.bfloat16)


def solution(mesh):
    split = Mesh(mesh.devices.reshape(2, 4, 4, 2, 2), ("z", "y", "x", "core", "head"))
    seq = ("z", "y", "x", "core")
    in_specs = (P(seq, "head"), P(seq, "head"), P(seq, "head"), P(seq), P("head", None))
    return jax.shard_map(
        shards, mesh=split, in_specs=in_specs, out_specs=P(seq, "head"), check_vma=False
    )
```

```python
import functools

import jax
import jax.numpy as jnp
import numpy as np
from jax import lax
from jax.experimental import pallas as pl
from jax.experimental.pallas import tpu as pltpu
from jax.sharding import Mesh, PartitionSpec as P

HD = 128
GROUP = 8
BLK = 96
ROWS = 200
QW = GROUP * BLK
SCALE = 1.4426950408889634 * HD**-0.5
LOWEST = -1e30
VMEM_BYTES = 24 << 20
TILE = 256
SUMS = HD + 8
HEADROOM = 60.0
UNROLL = 4
WCOLS = 512


def shifted(array, axis, by):
    size = lax.axis_size(axis)
    return lax.ppermute(array, axis, [(i, (i + by) % size) for i in range(size)])


def columns(start, size):
    return pl.ds(pl.multiple_of(start, HD), size)


def fold(scores, values, flags, cols, m_ref, o_ref):
    old = m_ref[:, cols]
    new = jnp.maximum(old, jnp.max(scores, axis=0, keepdims=True) * SCALE)
    weights = jnp.exp2(scores * SCALE - new).astype(jnp.bfloat16)
    m_ref[:, cols] = new
    terms = jnp.concatenate([values.T, flags], axis=0)
    o_ref[:, cols] = (
        o_ref[:, cols] * jnp.exp2(old - new)
        + jnp.dot(terms, weights, preferred_element_type=jnp.float32)[:SUMS]
    )


def list_steps(total, own, tag_ref, b_ref, lo_ref, hi_ref, lists):
    def write(step, *entries):
        for ref, entry in zip(lists, entries):
            ref[step] = jnp.asarray(entry, jnp.int32)

    half = total // 2
    for s in range(2):
        for p in range(half):
            write(s * half + p, 4 * p, 4 * p + 2, 4 * p, 4 * p + 2, 0, s * QW)
    for s in range(2):
        low_count = high_count = jnp.int32(0)
        for d in range(total):
            if own and d == s:
                continue
            low = jnp.where(tag_ref[d] < b_ref[s], 1, 0).astype(jnp.int32)
            lo_ref[low_count] = jnp.int32(2 * d)
            hi_ref[high_count] = jnp.int32(2 * d + 1)
            low_count = low_count + low
            high_count = high_count + (1 - low)
        low_steps = lax.div(low_count + 1, 2)

        def build(t, carry, s=s, low_count=low_count, high_count=high_count, low_steps=low_steps):
            is_low = t < low_steps
            u = 2 * jnp.where(is_low, t, t - low_steps)
            count = jnp.where(is_low, low_count, high_count)
            u0, u1 = jnp.minimum(u, total - 1), jnp.minimum(u + 1, total - 1)
            there, paired = u < count, u + 1 < count
            a0 = jnp.where(there, jnp.where(is_low, lo_ref[u0], hi_ref[u0]), 0)
            a1 = jnp.where(paired, jnp.where(is_low, lo_ref[u1], hi_ref[u1]), a0)
            nothing = 2 * total
            write(
                total + s * (half + 1) + t,
                a0,
                a1,
                jnp.where(there, a0, nothing),
                jnp.where(paired, a1, nothing),
                jnp.where(there, jnp.where(paired, 0, 1), 2),
                jnp.where(is_low, 2 * QW, 0) + s * QW,
            )
            return carry

        lax.fori_loop(0, half + 1, build, 0)


def attend_kernel(counts, first, last, *refs):
    number = len(counts)
    pieces = refs[:number]
    refs = refs[number:]
    if first:
        whole_ref, q_given = refs[:2]
        b_ref, q_out, m_ref, o_ref = refs[2:6]
        m_base, o_base, q_own, sem = refs[6:10]
        refs = refs[10:]
        q_refs = (q_own, q_given)
        width = GROUP * HD
        mine = pl.ds(pl.multiple_of(lax.axis_index("core") * width, HD), width)
        fetch = pltpu.make_async_copy(whole_ref.at[:, mine], q_own, sem)
        fetch.start()
    else:
        b_ref, q_in, m_base, o_base = refs[:4]
        if last:
            att_refs = refs[4:6]
            refs = refs[6:]
        else:
            refs = refs[4:]
        m_ref, o_ref = refs[:2]
        refs = refs[2:]
    kv_ref, qt_ref, flag_ref, x_ref, tag_ref, lo_ref, hi_ref = refs[:7]
    p_refs, lists = refs[7:9], refs[9:15]
    k0_ref, k1_ref, v0_ref, v1_ref, which_ref, col_ref = lists

    places = [(p, i * ROWS) for p, count in zip(pieces, counts) for i in range(count)]
    total = len(places)
    for i, (piece, base) in enumerate(places):
        tag_ref[i] = jnp.max(
            piece[base + 2 * BLK : base + 2 * BLK + 8, :HD].astype(jnp.float32)
        ).astype(jnp.int32)
        for half in range(2):
            kv_ref[2 * i + half] = piece[base + half * BLK : base + half * BLK + BLK, :]
    kv_ref[2 * total] = jnp.zeros((BLK, 2 * HD), jnp.bfloat16)
    lane = lax.broadcasted_iota(jnp.int32, (16, 2 * BLK), 1)
    for i, most in enumerate((2 * BLK, BLK, 0)):
        flag_ref[i] = jnp.where(lane < most, 1.0, 0.0).astype(jnp.bfloat16)

    if first:
        fetch.wait()
        for s in range(2):
            b_ref[s] = tag_ref[s]
            for half in range(2):
                rows = slice(half * BLK, half * BLK + BLK)
                tall = jnp.concatenate(
                    [q_refs[s][rows, h * HD : (h + 1) * HD] for h in range(GROUP)], axis=0
                )
                start = ((1 - half) * 2 + s) * QW
                qt_ref[:, start : start + QW] = tall.T
        q_out[...] = qt_ref[...]
        m_base[...] = jnp.full(m_base.shape, LOWEST, jnp.float32)
        o_base[...] = jnp.zeros(o_base.shape, jnp.float32)
        token = lax.rem(lax.broadcasted_iota(jnp.int32, (1, QW), 1), BLK)
        seen = lax.broadcasted_iota(jnp.int32, (BLK, QW), 0) <= token
        for s in range(2):
            for half in range(2):
                start = ((1 - half) * 2 + s) * QW
                cols = slice(start, start + QW)
                block = kv_ref[2 * s + half]
                scores = jnp.dot(block[:, :HD], qt_ref[:, cols], preferred_element_type=jnp.float32)
                scores = jnp.where(seen, scores, LOWEST)
                fold(scores, block[:, HD:], flag_ref[0][:, :BLK], cols, m_base, o_base)
    else:
        qt_ref[...] = q_in[...]
    list_steps(total, first, tag_ref, b_ref, lo_ref, hi_ref, lists)
    m_ref[...] = m_base[...]
    o_ref[...] = o_base[...]
    x_ref[...] = jnp.full(x_ref.shape, LOWEST, jnp.float32)

    def keys(step):
        return jnp.concatenate([kv_ref[k0_ref[step], :, :HD], kv_ref[k1_ref[step], :, :HD]], axis=0)

    def values(step):
        return jnp.concatenate([kv_ref[v0_ref[step], :, HD:], kv_ref[v1_ref[step], :, HD:]], axis=0)

    def weigh(step, slot):
        k = keys(step)
        for c in range(0, QW, TILE):
            cols = columns(col_ref[step] + c, TILE)
            scores = jnp.dot(k, qt_ref[:, cols], preferred_element_type=jnp.float32)
            p_refs[slot][:, c : c + TILE] = jnp.exp2(scores * SCALE - m_ref[:, cols]).astype(
                jnp.bfloat16
            )
            x_ref[:, cols] = jnp.maximum(
                x_ref[:, cols], jnp.max(scores.reshape(2 * BLK // 8, 8, TILE), axis=0)
            )

    def add(step, slot):
        terms = jnp.concatenate([values(step).T, flag_ref[which_ref[step]]], axis=0)
        for c in range(0, QW, TILE):
            cols = columns(col_ref[step] + c, TILE)
            o_ref[:, cols] += jnp.dot(
                terms, p_refs[slot][:, c : c + TILE], preferred_element_type=jnp.float32
            )[:SUMS]

    steps = 2 * total + 2

    def turn(j, carry):
        for i in range(UNROLL):
            weigh(UNROLL * j + 1 + i, 1 - i % 2)
            add(UNROLL * j + i, i % 2)
        return carry

    turns = (steps - 1) // UNROLL
    weigh(0, 0)
    lax.fori_loop(0, turns, turn, 0)
    for i in range(UNROLL * turns, steps):
        if i + 1 < steps:
            weigh(i + 1, 1 - i % 2)
        add(i, i % 2)

    @pl.when(jnp.max(x_ref[...] * SCALE - m_ref[...]) > HEADROOM)
    def _():
        m_ref[...] = m_base[...]
        o_ref[...] = o_base[...]

        def again(step, carry):
            cols = columns(col_ref[step], QW)
            scores = jnp.dot(keys(step), qt_ref[:, cols], preferred_element_type=jnp.float32)
            fold(scores, values(step), flag_ref[which_ref[step]], cols, m_ref, o_ref)
            return carry

        lax.fori_loop(0, steps, again, 0)

    if last:
        for s in range(2):
            for half in range(2):
                start = ((1 - half) * 2 + s) * QW
                cols = slice(start, start + QW)
                done = (o_ref[:HD, cols] / o_ref[HD : HD + 1, cols]).T
                for h in range(GROUP):
                    att_refs[s][half * BLK : (half + 1) * BLK, h * HD : (h + 1) * HD] = done[
                        h * BLK : (h + 1) * BLK
                    ].astype(jnp.bfloat16)


def attend(pieces, state, first=False, last=False):
    counts = tuple(p.shape[0] // ROWS for p in pieces)
    total = sum(counts)
    vmem = pl.BlockSpec(memory_space=pltpu.VMEM)
    smem = pl.BlockSpec(memory_space=pltpu.SMEM)
    width = 4 * QW
    kept = [
        jax.ShapeDtypeStruct((1, width), jnp.float32),
        jax.ShapeDtypeStruct((SUMS, width), jnp.float32),
    ]
    scratch = []
    in_specs = [vmem] * (len(pieces) + len(state))
    if first:
        outs = [
            jax.ShapeDtypeStruct((2,), jnp.int32),
            jax.ShapeDtypeStruct((HD, width), jnp.bfloat16),
        ] + kept
        out_specs = [smem] + [vmem] * 3
        scratch = [pltpu.VMEM(k.shape, k.dtype) for k in kept]
        scratch += [pltpu.VMEM((2 * BLK, GROUP * HD), jnp.bfloat16), pltpu.SemaphoreType.DMA]
        in_specs[len(pieces)] = pl.BlockSpec(memory_space=pltpu.HBM)
    else:
        outs = [jax.ShapeDtypeStruct((2 * BLK, GROUP * HD), jnp.bfloat16)] * (2 * last) + kept
        out_specs = [vmem] * len(outs)
        in_specs[len(pieces)] = smem
    cells = total * 2 * BLK * BLK * 2 * GROUP
    return pl.pallas_call(
        functools.partial(attend_kernel, counts, first, last),
        out_shape=outs,
        in_specs=in_specs,
        out_specs=out_specs,
        scratch_shapes=scratch
        + [
            pltpu.VMEM((2 * total + 1, BLK, 2 * HD), jnp.bfloat16),
            pltpu.VMEM((HD, width), jnp.bfloat16),
            pltpu.VMEM((3, 16, 2 * BLK), jnp.bfloat16),
            pltpu.VMEM((8, width), jnp.float32),
        ]
        + [pltpu.SMEM((total + 1,), jnp.int32)] * 3
        + [pltpu.VMEM((2 * BLK, QW), jnp.bfloat16)] * 2
        + [pltpu.SMEM((2 * total + 2,), jnp.int32)] * 6,
        cost_estimate=pl.CostEstimate(
            flops=4 * HD * cells, transcendentals=cells, bytes_accessed=total * ROWS * 512
        ),
        compiler_params=pltpu.CompilerParams(vmem_limit_bytes=VMEM_BYTES),
    )(*pieces, *state)


def pack_kernel(place_ref, k_ref, v_ref, own_ref, sent_ref, first_ref, sems):
    core = lax.axis_index("core")
    place = pltpu.make_async_copy(place_ref.at[pl.ds(0, 128)], first_ref, sems.at[4])
    place.start()
    copies = []
    for which, to_ref in ((1 - core, sent_ref), (core, own_ref)):
        cols = pl.ds(pl.multiple_of(which * HD, HD), HD)
        for from_ref, at in ((k_ref, 0), (v_ref, HD)):
            copies.append(
                pltpu.make_async_copy(
                    from_ref.at[:, cols],
                    to_ref.at[pl.ds(0, 2 * BLK), pl.ds(at, HD)],
                    sems.at[len(copies)],
                )
            )
    for copy in copies:
        copy.start()
    place.wait()
    tag = lax.div(first_ref[0], BLK).astype(jnp.float32)
    tags = jnp.full((ROWS - 2 * BLK, 2 * HD), tag, jnp.float32).astype(jnp.bfloat16)
    own_ref[2 * BLK :, :] = tags
    sent_ref[2 * BLK :, :] = tags
    for copy in copies:
        copy.wait()


def pack(positions, keys, values):
    vmem = pl.BlockSpec(memory_space=pltpu.VMEM)
    anywhere = pl.BlockSpec(memory_space=pltpu.HBM)
    kv = jax.ShapeDtypeStruct((ROWS, 2 * HD), jnp.bfloat16)
    return pl.pallas_call(
        pack_kernel,
        out_shape=[kv, kv],
        in_specs=[anywhere] * 3,
        out_specs=[vmem] * 2,
        scratch_shapes=[pltpu.SMEM((128,), jnp.int32), pltpu.SemaphoreType.DMA((5,))],
        compiler_params=pltpu.CompilerParams(vmem_limit_bytes=VMEM_BYTES),
    )(positions, keys, values)


def query_kernel(q_ref, sent_ref, sem):
    width = GROUP * HD
    cols = pl.ds(pl.multiple_of((1 - lax.axis_index("core")) * width, HD), width)
    copy = pltpu.make_async_copy(q_ref.at[:, cols], sent_ref, sem)
    copy.start()
    copy.wait()


def queries_for_partner(queries):
    return pl.pallas_call(
        query_kernel,
        out_shape=jax.ShapeDtypeStruct((2 * BLK, GROUP * HD), jnp.bfloat16),
        in_specs=[pl.BlockSpec(memory_space=pltpu.HBM)],
        out_specs=pl.BlockSpec(memory_space=pl.ANY),
        scratch_shapes=[pltpu.SemaphoreType.DMA],
        compiler_params=pltpu.CompilerParams(vmem_limit_bytes=VMEM_BYTES),
    )(queries)


def join_kernel(number, *refs):
    parts, whole, sems = refs[:number], refs[number], refs[number + 1]
    copies, at = [], 0
    for i, part in enumerate(parts):
        rows = part.shape[0]
        copies.append(pltpu.make_async_copy(part, whole.at[pl.ds(at, rows)], sems.at[i]))
        at += rows
    for copy in copies:
        copy.start()
    for copy in copies:
        copy.wait()


def joined(parts):
    rows = sum(p.shape[0] for p in parts)
    anywhere = pl.BlockSpec(memory_space=pl.ANY)
    return pl.pallas_call(
        functools.partial(join_kernel, len(parts)),
        out_shape=jax.ShapeDtypeStruct((rows, parts[0].shape[1]), parts[0].dtype),
        in_specs=[anywhere] * len(parts),
        out_specs=anywhere,
        scratch_shapes=[pltpu.SemaphoreType.DMA((len(parts),))],
        compiler_params=pltpu.CompilerParams(vmem_limit_bytes=VMEM_BYTES),
    )(*parts)


def near(array, axis):
    return [shifted(array, axis, 1), shifted(array, axis, -1)]


def far(pair, axis):
    half = pair[0].shape[0] // 2
    return [shifted(pair[0][:half], axis, 1), shifted(pair[1][half:], axis, -1)]


def after(pairs, token):
    *arrays, _ = lax.optimization_barrier((*sum(pairs, []), token))
    return [arrays[i : i + 2] for i in range(0, len(arrays), 2)]


def project_kernel(others, theirs, start, size, with_sum, *refs):
    number = len(others)
    att_refs, w_ref = refs[:number], refs[number]
    w_buf, sems = refs[-2:]
    out_ref = refs[-3]
    core, head = lax.axis_index("core"), lax.axis_index("head")
    rows = w_ref.shape[0] // 2
    half = w_ref.shape[1] // 2
    side = 1 - head if theirs else head
    blocks = size // WCOLS
    copies = []
    for j in range(blocks):
        for i, other in enumerate(others):
            row = (1 - core if other else core) * rows
            col = side * half + start + j * WCOLS
            at = j * number + i
            copies.append(
                pltpu.make_async_copy(
                    w_ref.at[
                        pl.ds(pl.multiple_of(row, rows), rows),
                        pl.ds(pl.multiple_of(col, WCOLS), WCOLS),
                    ],
                    w_buf.at[at],
                    sems.at[at],
                )
            )
    for copy in copies:
        copy.start()
    for j in range(blocks):
        cols = slice(j * WCOLS, (j + 1) * WCOLS)
        total = refs[number + 1][:, start + j * WCOLS : start + (j + 1) * WCOLS] if with_sum else 0.0
        for i, att_ref in enumerate(att_refs):
            copies[j * number + i].wait()
            total = total + jnp.dot(
                att_ref[...], w_buf[j * number + i], preferred_element_type=jnp.float32
            )
        out_ref[:, cols] = total.astype(out_ref.dtype)


def project(atts, others, weight, theirs, start, size, dtype, total=None):
    vmem = pl.BlockSpec(memory_space=pltpu.VMEM)
    rows, width = atts[0].shape
    pieces = len(atts) * size // WCOLS
    sums = [] if total is None else [total]
    return pl.pallas_call(
        functools.partial(project_kernel, others, theirs, start, size, total is not None),
        in_specs=[vmem] * len(atts) + [pl.BlockSpec(memory_space=pltpu.HBM)] + [vmem] * len(sums),
        out_specs=vmem,
        out_shape=jax.ShapeDtypeStruct((rows, size), dtype),
        scratch_shapes=[
            pltpu.VMEM((pieces, width, WCOLS), jnp.bfloat16),
            pltpu.SemaphoreType.DMA((pieces,)),
        ],
        cost_estimate=pl.CostEstimate(
            flops=2 * rows * width * len(atts) * size,
            transcendentals=0,
            bytes_accessed=2 * width * len(atts) * size,
        ),
        compiler_params=pltpu.CompilerParams(vmem_limit_bytes=VMEM_BYTES),
    )(*atts, weight, *sums)


def shards(queries, key_states, value_states, positions, out_weight):
    own, sent = pack(positions, key_states, value_states)
    both = joined([own, shifted(sent, "core", 1)])
    q_given = shifted(queries_for_partner(queries), "core", 1)

    beyond = shifted(both, "z", 1)
    near_a, near_b = near(both, "x"), near(beyond, "y")
    b_both, qt, *state = attend([both, beyond], [queries, q_given], first=True)
    near_a, near_b = after([near_a, near_b], state[0])
    far_a, far_b = far(near_a, "x"), far(near_b, "y")
    pieces = near_a + near_b + far_a + far_b
    all_a = joined([both] + near_a + far_a)
    all_b = joined([beyond] + near_b + far_b)
    near_a, near_b = near(all_a, "y"), near(all_b, "x")
    state = attend(pieces, [b_both, qt, *state])
    near_a, near_b = after([near_a, near_b], state[0])
    far_a, far_b = far(near_a, "y"), far(near_b, "x")
    state = attend(near_a + near_b, [b_both, qt, *state])
    mine, returned = attend(far_a + far_b, [b_both, qt, *state], last=True)[:2]

    returned = shifted(returned, "core", 1)
    half = out_weight.shape[1] // 2
    sums = project([mine], [False], out_weight, True, 0, half, jnp.float32)
    swapped = []
    for start in range(0, half, half // 2):
        given = project([returned], [True], out_weight, True, start, half // 2, jnp.bfloat16, sums)
        swapped.append(shifted(given, "head", 1))
    kept = project([mine, returned], [False, True], out_weight, False, 0, half, jnp.float32)
    return (kept + jnp.concatenate(swapped, axis=1).astype(jnp.float32)).astype(jnp.bfloat16)


def solution(mesh):
    split = Mesh(mesh.devices.reshape(2, 4, 4, 2, 2), ("z", "y", "x", "core", "head"))
    seq = ("z", "y", "x", "core")
    in_specs = (P(seq, "head"), P(seq, "head"), P(seq, "head"), P(seq), P("head", None))
    return jax.shard_map(
        shards, mesh=split, in_specs=in_specs, out_specs=P(seq, "head"), check_vma=False
    )
```

```python
import functools

import jax
import jax.numpy as jnp
import numpy as np
from jax import lax
from jax.experimental import pallas as pl
from jax.experimental.pallas import tpu as pltpu
from jax.sharding import Mesh, PartitionSpec as P

HD = 128
GROUP = 8
BLK = 96
ROWS = 200
QW = GROUP * BLK
SCALE = 1.4426950408889634 * HD**-0.5
LOWEST = -1e30
VMEM_BYTES = 24 << 20
TILE = 768
SUMS = HD + 8
HEADROOM = 60.0
UNROLL = 8
WCOLS = 512


def shifted(array, axis, by):
    size = lax.axis_size(axis)
    return lax.ppermute(array, axis, [(i, (i + by) % size) for i in range(size)])


def columns(start, size):
    return pl.ds(pl.multiple_of(start, HD), size)


def fold(scores, values, flags, cols, m_ref, o_ref):
    old = m_ref[:, cols]
    new = jnp.maximum(old, jnp.max(scores, axis=0, keepdims=True) * SCALE)
    weights = jnp.exp2(scores * SCALE - new).astype(jnp.bfloat16)
    m_ref[:, cols] = new
    terms = jnp.concatenate([values.T, flags], axis=0)
    o_ref[:, cols] = (
        o_ref[:, cols] * jnp.exp2(old - new)
        + jnp.dot(terms, weights, preferred_element_type=jnp.float32)[:SUMS]
    )


def list_steps(total, tag_ref, b_ref, lo_ref, hi_ref, lists):
    def write(step, *entries):
        for ref, entry in zip(lists, entries):
            ref[step] = jnp.asarray(entry, jnp.int32)

    half = total // 2
    for s in range(2):
        for p in range(half):
            write(s * half + p, 4 * p, 4 * p + 2, 4 * p, 4 * p + 2, 0, s * QW)
    for s in range(2):
        low_count = high_count = jnp.int32(0)
        for d in range(total):
            low = jnp.where(tag_ref[d] < b_ref[s], 1, 0).astype(jnp.int32)
            high = jnp.where(tag_ref[d] > b_ref[s], 1, 0).astype(jnp.int32)
            lo_ref[low_count] = jnp.int32(2 * d)
            hi_ref[high_count] = jnp.int32(2 * d + 1)
            low_count = low_count + low
            high_count = high_count + high
        low_steps = lax.div(low_count + 1, 2)

        def build(t, carry, s=s, low_count=low_count, high_count=high_count, low_steps=low_steps):
            is_low = t < low_steps
            u = 2 * jnp.where(is_low, t, t - low_steps)
            count = jnp.where(is_low, low_count, high_count)
            u0, u1 = jnp.minimum(u, total - 1), jnp.minimum(u + 1, total - 1)
            there, paired = u < count, u + 1 < count
            a0 = jnp.where(there, jnp.where(is_low, lo_ref[u0], hi_ref[u0]), 0)
            a1 = jnp.where(paired, jnp.where(is_low, lo_ref[u1], hi_ref[u1]), a0)
            nothing = 2 * total
            write(
                total + s * (half + 1) + t,
                a0,
                a1,
                jnp.where(there, a0, nothing),
                jnp.where(paired, a1, nothing),
                jnp.where(there, jnp.where(paired, 0, 1), 2),
                jnp.where(is_low, 2 * QW, 0) + s * QW,
            )
            return carry

        lax.fori_loop(0, half + 1, build, 0)


def tag_of(piece, base):
    rows = piece[base + 2 * BLK : base + 2 * BLK + 8, :HD]
    return jnp.max(rows.astype(jnp.float32)).astype(jnp.int32)


def begin_kernel(both_ref, whole_ref, q_given, b_ref, qt_ref, m_ref, o_ref, q_own, flag_ref, sem):
    width = GROUP * HD
    mine = pl.ds(pl.multiple_of(lax.axis_index("core") * width, HD), width)
    fetch = pltpu.make_async_copy(whole_ref.at[:, mine], q_own, sem)
    fetch.start()
    m_ref[...] = jnp.full(m_ref.shape, LOWEST, jnp.float32)
    o_ref[...] = jnp.zeros(o_ref.shape, jnp.float32)
    flag_ref[...] = jnp.ones(flag_ref.shape, jnp.bfloat16)
    token = lax.rem(lax.broadcasted_iota(jnp.int32, (1, QW), 1), BLK)
    seen = lax.broadcasted_iota(jnp.int32, (BLK, QW), 0) <= token
    fetch.wait()
    for s in range(2):
        base = s * ROWS
        b_ref[s] = tag_of(both_ref, base)
        for half in range(2):
            rows = slice(half * BLK, half * BLK + BLK)
            q_ref = (q_own, q_given)[s]
            tall = jnp.concatenate([q_ref[rows, h * HD : (h + 1) * HD] for h in range(GROUP)], axis=0)
            start = ((1 - half) * 2 + s) * QW
            cols = slice(start, start + QW)
            qt_ref[:, cols] = tall.T
            block = both_ref[base + half * BLK : base + half * BLK + BLK, :]
            scores = jnp.dot(block[:, :HD], qt_ref[:, cols], preferred_element_type=jnp.float32)
            scores = jnp.where(seen, scores, LOWEST)
            fold(scores, block[:, HD:], flag_ref[...], cols, m_ref, o_ref)


def begin(both, queries, q_given):
    vmem = pl.BlockSpec(memory_space=pltpu.VMEM)
    width = 4 * QW
    return pl.pallas_call(
        begin_kernel,
        out_shape=[
            jax.ShapeDtypeStruct((2,), jnp.int32),
            jax.ShapeDtypeStruct((HD, width), jnp.bfloat16),
            jax.ShapeDtypeStruct((1, width), jnp.float32),
            jax.ShapeDtypeStruct((SUMS, width), jnp.float32),
        ],
        in_specs=[vmem, pl.BlockSpec(memory_space=pltpu.HBM), vmem],
        out_specs=[pl.BlockSpec(memory_space=pltpu.SMEM)] + [vmem] * 3,
        scratch_shapes=[
            pltpu.VMEM((2 * BLK, GROUP * HD), jnp.bfloat16),
            pltpu.VMEM((16, BLK), jnp.bfloat16),
            pltpu.SemaphoreType.DMA,
        ],
        cost_estimate=pl.CostEstimate(
            flops=16 * HD * BLK * QW, transcendentals=4 * BLK * QW, bytes_accessed=1 << 20
        ),
        compiler_params=pltpu.CompilerParams(vmem_limit_bytes=VMEM_BYTES),
    )(both, queries, q_given)


def attend_kernel(counts, last, *refs):
    number = len(counts)
    pieces = refs[:number]
    refs = refs[number:]
    b_ref, q_in, m_base, o_base = refs[:4]
    if last:
        att_refs = refs[4:6]
        m_ref, o_ref = refs[6:8]
        refs = refs[8:]
    else:
        m_ref, o_ref = refs[4:6]
        refs = refs[6:]
    kv_ref, qt_ref, flag_ref, x_ref, tag_ref, lo_ref, hi_ref = refs[:7]
    p_refs, lists = refs[7:9], refs[9:15]
    k0_ref, k1_ref, v0_ref, v1_ref, which_ref, col_ref = lists

    places = [(p, i * ROWS) for p, count in zip(pieces, counts) for i in range(count)]
    total = len(places)
    for i, (piece, base) in enumerate(places):
        tag_ref[i] = tag_of(piece, base)
        for half in range(2):
            kv_ref[2 * i + half] = piece[base + half * BLK : base + half * BLK + BLK, :]
    kv_ref[2 * total] = jnp.zeros((BLK, 2 * HD), jnp.bfloat16)
    lane = lax.broadcasted_iota(jnp.int32, (16, 2 * BLK), 1)
    for i, most in enumerate((2 * BLK, BLK, 0)):
        flag_ref[i] = jnp.where(lane < most, 1.0, 0.0).astype(jnp.bfloat16)

    qt_ref[...] = q_in[...]
    list_steps(total, tag_ref, b_ref, lo_ref, hi_ref, lists)
    m_ref[...] = m_base[...]
    o_ref[...] = o_base[...]
    x_ref[...] = jnp.full(x_ref.shape, LOWEST, jnp.float32)

    def keys(step):
        return jnp.concatenate([kv_ref[k0_ref[step], :, :HD], kv_ref[k1_ref[step], :, :HD]], axis=0)

    def values(step):
        return jnp.concatenate([kv_ref[v0_ref[step], :, HD:], kv_ref[v1_ref[step], :, HD:]], axis=0)

    def weigh(step, slot):
        k = keys(step)
        for c in range(0, QW, TILE):
            cols = columns(col_ref[step] + c, TILE)
            scores = jnp.dot(k, qt_ref[:, cols], preferred_element_type=jnp.float32)
            p_refs[slot][:, c : c + TILE] = jnp.exp2(scores * SCALE - m_ref[:, cols]).astype(
                jnp.bfloat16
            )
            x_ref[:, cols] = jnp.maximum(
                x_ref[:, cols], jnp.max(scores.reshape(2 * BLK // 8, 8, TILE), axis=0)
            )

    def add(step, slot):
        terms = jnp.concatenate([values(step).T, flag_ref[which_ref[step]]], axis=0)
        for c in range(0, QW, TILE):
            cols = columns(col_ref[step] + c, TILE)
            o_ref[:, cols] += jnp.dot(
                terms, p_refs[slot][:, c : c + TILE], preferred_element_type=jnp.float32
            )[:SUMS]

    steps = 2 * total + 2

    def turn(j, carry):
        for i in range(UNROLL):
            weigh(UNROLL * j + 1 + i, 1 - i % 2)
            add(UNROLL * j + i, i % 2)
        return carry

    turns = (steps - 1) // UNROLL
    weigh(0, 0)
    lax.fori_loop(0, turns, turn, 0)
    for i in range(UNROLL * turns, steps):
        if i + 1 < steps:
            weigh(i + 1, 1 - i % 2)
        add(i, i % 2)

    @pl.when(jnp.max(x_ref[...] * SCALE - m_ref[...]) > HEADROOM)
    def _():
        m_ref[...] = m_base[...]
        o_ref[...] = o_base[...]

        def again(step, carry):
            cols = columns(col_ref[step], QW)
            scores = jnp.dot(keys(step), qt_ref[:, cols], preferred_element_type=jnp.float32)
            fold(scores, values(step), flag_ref[which_ref[step]], cols, m_ref, o_ref)
            return carry

        lax.fori_loop(0, steps, again, 0)

    if last:
        for s in range(2):
            for half in range(2):
                start = ((1 - half) * 2 + s) * QW
                cols = slice(start, start + QW)
                done = (o_ref[:HD, cols] / o_ref[HD : HD + 1, cols]).T
                for h in range(GROUP):
                    att_refs[s][half * BLK : (half + 1) * BLK, h * HD : (h + 1) * HD] = done[
                        h * BLK : (h + 1) * BLK
                    ].astype(jnp.bfloat16)


def attend(pieces, state, last=False):
    counts = tuple(p.shape[0] // ROWS for p in pieces)
    total = sum(counts)
    vmem = pl.BlockSpec(memory_space=pltpu.VMEM)
    smem = pl.BlockSpec(memory_space=pltpu.SMEM)
    width = 4 * QW
    kept = [(1, width), (SUMS, width)]
    if last:
        outs = [jax.ShapeDtypeStruct((2 * BLK, GROUP * HD), jnp.bfloat16)] * 2
        scratch = [pltpu.VMEM(shape, jnp.float32) for shape in kept]
    else:
        outs = [jax.ShapeDtypeStruct(shape, jnp.float32) for shape in kept]
        scratch = []
    in_specs = [vmem] * len(pieces) + [smem] + [vmem] * 3
    cells = total * 2 * BLK * BLK * 2 * GROUP
    return pl.pallas_call(
        functools.partial(attend_kernel, counts, last),
        out_shape=outs,
        in_specs=in_specs,
        out_specs=[vmem] * 2,
        scratch_shapes=scratch
        + [
            pltpu.VMEM((2 * total + 1, BLK, 2 * HD), jnp.bfloat16),
            pltpu.VMEM((HD, width), jnp.bfloat16),
            pltpu.VMEM((3, 16, 2 * BLK), jnp.bfloat16),
            pltpu.VMEM((8, width), jnp.float32),
        ]
        + [pltpu.SMEM((total + 1,), jnp.int32)] * 3
        + [pltpu.VMEM((2 * BLK, QW), jnp.bfloat16)] * 2
        + [pltpu.SMEM((2 * total + 2,), jnp.int32)] * 6,
        cost_estimate=pl.CostEstimate(
            flops=4 * HD * cells, transcendentals=cells, bytes_accessed=total * ROWS * 512
        ),
        compiler_params=pltpu.CompilerParams(vmem_limit_bytes=VMEM_BYTES),
    )(*pieces, *state)


def join_kernel(number, *refs):
    parts, whole, sems = refs[:number], refs[number], refs[number + 1]
    copies, at = [], 0
    for i, part in enumerate(parts):
        rows = part.shape[0]
        copies.append(pltpu.make_async_copy(part, whole.at[pl.ds(at, rows)], sems.at[i]))
        at += rows
    for copy in copies:
        copy.start()
    for copy in copies:
        copy.wait()


def joined(parts):
    rows = sum(p.shape[0] for p in parts)
    anywhere = pl.BlockSpec(memory_space=pl.ANY)
    return pl.pallas_call(
        functools.partial(join_kernel, len(parts)),
        out_shape=jax.ShapeDtypeStruct((rows, parts[0].shape[1]), parts[0].dtype),
        in_specs=[anywhere] * len(parts),
        out_specs=anywhere,
        scratch_shapes=[pltpu.SemaphoreType.DMA((len(parts),))],
        compiler_params=pltpu.CompilerParams(vmem_limit_bytes=VMEM_BYTES),
    )(*parts)


def near(array, axis):
    return [shifted(array, axis, 1), shifted(array, axis, -1)]


def far(pair, axis):
    half = pair[0].shape[0] // 2
    return [shifted(pair[0][:half], axis, 1), shifted(pair[1][half:], axis, -1)]


def after(pairs, token):
    *arrays, _ = lax.optimization_barrier((*sum(pairs, []), token))
    return [arrays[i : i + 2] for i in range(0, len(arrays), 2)]


def project_kernel(others, theirs, start, size, with_sum, *refs):
    number = len(others)
    att_refs, w_ref = refs[:number], refs[number]
    w_buf, sems = refs[-2:]
    out_ref = refs[-3]
    core, head = lax.axis_index("core"), lax.axis_index("head")
    rows = w_ref.shape[0] // 2
    half = w_ref.shape[1] // 2
    side = 1 - head if theirs else head
    blocks = size // WCOLS
    copies = []
    for j in range(blocks):
        for i, other in enumerate(others):
            row = (1 - core if other else core) * rows
            col = side * half + start + j * WCOLS
            at = j * number + i
            copies.append(
                pltpu.make_async_copy(
                    w_ref.at[
                        pl.ds(pl.multiple_of(row, rows), rows),
                        pl.ds(pl.multiple_of(col, WCOLS), WCOLS),
                    ],
                    w_buf.at[at],
                    sems.at[at],
                )
            )
    for copy in copies:
        copy.start()
    for j in range(blocks):
        cols = slice(j * WCOLS, (j + 1) * WCOLS)
        total = refs[number + 1][:, start + j * WCOLS : start + (j + 1) * WCOLS] if with_sum else 0.0
        for i, att_ref in enumerate(att_refs):
            copies[j * number + i].wait()
            total = total + jnp.dot(
                att_ref[...], w_buf[j * number + i], preferred_element_type=jnp.float32
            )
        out_ref[:, cols] = total.astype(out_ref.dtype)


def project(atts, others, weight, theirs, start, size, dtype, total=None):
    vmem = pl.BlockSpec(memory_space=pltpu.VMEM)
    rows, width = atts[0].shape
    pieces = len(atts) * size // WCOLS
    sums = [] if total is None else [total]
    return pl.pallas_call(
        functools.partial(project_kernel, others, theirs, start, size, total is not None),
        in_specs=[vmem] * len(atts) + [pl.BlockSpec(memory_space=pltpu.HBM)] + [vmem] * len(sums),
        out_specs=vmem,
        out_shape=jax.ShapeDtypeStruct((rows, size), dtype),
        scratch_shapes=[
            pltpu.VMEM((pieces, width, WCOLS), jnp.bfloat16),
            pltpu.SemaphoreType.DMA((pieces,)),
        ],
        cost_estimate=pl.CostEstimate(
            flops=2 * rows * width * len(atts) * size,
            transcendentals=0,
            bytes_accessed=2 * width * len(atts) * size,
        ),
        compiler_params=pltpu.CompilerParams(vmem_limit_bytes=VMEM_BYTES),
    )(*atts, weight, *sums)


def shards(queries, key_states, value_states, positions, out_weight):
    first_core = lax.axis_index("core") == 0
    tag = lax.div(positions[0], BLK).astype(jnp.bfloat16)

    def packed(low):
        parts = [jnp.where(low, a[:, :HD], a[:, HD:]) for a in (key_states, value_states)]
        return jnp.pad(
            jnp.concatenate(parts, axis=1), ((0, ROWS - 2 * BLK), (0, 0)), constant_values=tag
        )

    given = shifted(packed(~first_core), "core", 1)
    both = joined([packed(first_core), given])
    whole, _ = lax.optimization_barrier((queries, both))
    width = GROUP * HD
    q_given = shifted(jnp.where(first_core, whole[:, width:], whole[:, :width]), "core", 1)

    beyond = shifted(both, "z", 1)
    near_a = near(both, "x")
    b_both, qt, *state = begin(both, queries, q_given)
    near_b = near(beyond, "y")
    far_a, far_b = far(near_a, "x"), far(near_b, "y")
    all_a = joined([both] + near_a + far_a)
    all_b = joined([beyond] + near_b + far_b)
    near_a, near_b = near(all_a, "y"), near(all_b, "x")
    state = attend([all_a, all_b], [b_both, qt, *state])
    near_a, near_b = after([near_a, near_b], state[0])
    far_a, far_b = far(near_a, "y"), far(near_b, "x")
    state = attend(near_a + near_b, [b_both, qt, *state])
    mine, returned = attend(far_a + far_b, [b_both, qt, *state], last=True)[:2]

    returned = shifted(returned, "core", 1)
    half = out_weight.shape[1] // 2
    sums = project([mine], [False], out_weight, True, 0, half, jnp.float32)
    swapped = []
    for start in range(0, half, half // 2):
        given = project([returned], [True], out_weight, True, start, half // 2, jnp.bfloat16, sums)
        swapped.append(shifted(given, "head", 1))
    kept = project([mine, returned], [False, True], out_weight, False, 0, half, jnp.float32)
    return (kept + jnp.concatenate(swapped, axis=1).astype(jnp.float32)).astype(jnp.bfloat16)


def solution(mesh):
    split = Mesh(mesh.devices.reshape(2, 4, 4, 2, 2), ("z", "y", "x", "core", "head"))
    seq = ("z", "y", "x", "core")
    in_specs = (P(seq, "head"), P(seq, "head"), P(seq, "head"), P(seq), P("head", None))
    return jax.shard_map(
        shards, mesh=split, in_specs=in_specs, out_specs=P(seq, "head"), check_vma=False
    )
```

```python
import functools

import jax
import jax.numpy as jnp
import numpy as np
from jax import lax
from jax.experimental import pallas as pl
from jax.experimental.pallas import tpu as pltpu
from jax.sharding import Mesh, PartitionSpec as P

HD = 128
GROUP = 8
BLK = 96
ROWS = 200
QW = GROUP * BLK
SCALE = 1.4426950408889634 * HD**-0.5
LOWEST = -1e30
VMEM_BYTES = 24 << 20
FETCH_VMEM_BYTES = 30 << 20
KEEP_VMEM_BYTES = 48 << 20
TILE = 768
SUMS = HD + 8
HEADROOM = 60.0
UNROLL = 8
WCOLS = 512


def shifted(array, axis, by):
    size = lax.axis_size(axis)
    return lax.ppermute(array, axis, [(i, (i + by) % size) for i in range(size)])


def columns(start, size):
    return pl.ds(pl.multiple_of(start, HD), size)


def fold(scores, values, flags, cols, m_ref, o_ref):
    old = m_ref[:, cols]
    new = jnp.maximum(old, jnp.max(scores, axis=0, keepdims=True) * SCALE)
    weights = jnp.exp2(scores * SCALE - new).astype(jnp.bfloat16)
    m_ref[:, cols] = new
    terms = jnp.concatenate([values.T, flags], axis=0)
    o_ref[:, cols] = (
        o_ref[:, cols] * jnp.exp2(old - new)
        + jnp.dot(terms, weights, preferred_element_type=jnp.float32)[:SUMS]
    )


def list_steps(total, tag_ref, b_ref, lo_ref, hi_ref, lists):
    def write(step, *entries):
        for ref, entry in zip(lists, entries):
            ref[step] = jnp.asarray(entry, jnp.int32)

    half = total // 2
    for s in range(2):
        for p in range(half):
            write(s * half + p, 4 * p, 4 * p + 2, 4 * p, 4 * p + 2, 0, s * QW)
    for s in range(2):
        low_count = high_count = jnp.int32(0)
        for d in range(total):
            low = jnp.where(tag_ref[d] < b_ref[s], 1, 0).astype(jnp.int32)
            high = jnp.where(tag_ref[d] > b_ref[s], 1, 0).astype(jnp.int32)
            lo_ref[low_count] = jnp.int32(2 * d)
            hi_ref[high_count] = jnp.int32(2 * d + 1)
            low_count = low_count + low
            high_count = high_count + high
        low_steps = lax.div(low_count + 1, 2)

        def build(t, carry, s=s, low_count=low_count, high_count=high_count, low_steps=low_steps):
            is_low = t < low_steps
            u = 2 * jnp.where(is_low, t, t - low_steps)
            count = jnp.where(is_low, low_count, high_count)
            u0, u1 = jnp.minimum(u, total - 1), jnp.minimum(u + 1, total - 1)
            there, paired = u < count, u + 1 < count
            a0 = jnp.where(there, jnp.where(is_low, lo_ref[u0], hi_ref[u0]), 0)
            a1 = jnp.where(paired, jnp.where(is_low, lo_ref[u1], hi_ref[u1]), a0)
            nothing = 2 * total
            write(
                total + s * (half + 1) + t,
                a0,
                a1,
                jnp.where(there, a0, nothing),
                jnp.where(paired, a1, nothing),
                jnp.where(there, jnp.where(paired, 0, 1), 2),
                jnp.where(is_low, 2 * QW, 0) + s * QW,
            )
            return carry

        lax.fori_loop(0, half + 1, build, 0)


def tag_of(piece, base):
    rows = piece[base + 2 * BLK : base + 2 * BLK + 8, :HD]
    return jnp.max(rows.astype(jnp.float32)).astype(jnp.int32)


def begin_kernel(both_ref, whole_ref, q_given, b_ref, qt_ref, m_ref, o_ref, q_own, flag_ref, sem):
    width = GROUP * HD
    mine = pl.ds(pl.multiple_of(lax.axis_index("core") * width, HD), width)
    fetch = pltpu.make_async_copy(whole_ref.at[:, mine], q_own, sem)
    fetch.start()
    m_ref[...] = jnp.full(m_ref.shape, LOWEST, jnp.float32)
    o_ref[...] = jnp.zeros(o_ref.shape, jnp.float32)
    flag_ref[...] = jnp.ones(flag_ref.shape, jnp.bfloat16)
    token = lax.rem(lax.broadcasted_iota(jnp.int32, (1, QW), 1), BLK)
    seen = lax.broadcasted_iota(jnp.int32, (BLK, QW), 0) <= token
    fetch.wait()
    for s in range(2):
        base = s * ROWS
        b_ref[s] = tag_of(both_ref, base)
        for half in range(2):
            rows = slice(half * BLK, half * BLK + BLK)
            q_ref = (q_own, q_given)[s]
            tall = jnp.concatenate([q_ref[rows, h * HD : (h + 1) * HD] for h in range(GROUP)], axis=0)
            start = ((1 - half) * 2 + s) * QW
            cols = slice(start, start + QW)
            qt_ref[:, cols] = tall.T
            block = both_ref[base + half * BLK : base + half * BLK + BLK, :]
            scores = jnp.dot(block[:, :HD], qt_ref[:, cols], preferred_element_type=jnp.float32)
            scores = jnp.where(seen, scores, LOWEST)
            fold(scores, block[:, HD:], flag_ref[...], cols, m_ref, o_ref)


def begin(both, queries, q_given):
    vmem = pl.BlockSpec(memory_space=pltpu.VMEM)
    width = 4 * QW
    return pl.pallas_call(
        begin_kernel,
        out_shape=[
            jax.ShapeDtypeStruct((2,), jnp.int32),
            jax.ShapeDtypeStruct((HD, width), jnp.bfloat16),
            jax.ShapeDtypeStruct((1, width), jnp.float32),
            jax.ShapeDtypeStruct((SUMS, width), jnp.float32),
        ],
        in_specs=[vmem, pl.BlockSpec(memory_space=pltpu.HBM), vmem],
        out_specs=[pl.BlockSpec(memory_space=pltpu.SMEM)] + [vmem] * 3,
        scratch_shapes=[
            pltpu.VMEM((2 * BLK, GROUP * HD), jnp.bfloat16),
            pltpu.VMEM((16, BLK), jnp.bfloat16),
            pltpu.SemaphoreType.DMA,
        ],
        cost_estimate=pl.CostEstimate(
            flops=16 * HD * BLK * QW, transcendentals=4 * BLK * QW, bytes_accessed=1 << 20
        ),
        compiler_params=pltpu.CompilerParams(vmem_limit_bytes=VMEM_BYTES),
    )(both, queries, q_given)


def attend_kernel(counts, last, fetch, *refs):
    number = len(counts)
    pieces = refs[:number]
    refs = refs[number:]
    b_ref, q_in, m_base, o_base = refs[:4]
    refs = refs[4:]
    if fetch:
        w_ref, m_ref, o_ref, w_out = refs[:4]
        refs, sem = refs[4:-1], refs[-1]
        size = w_out.shape[1]
        start = pl.multiple_of((1 - lax.axis_index("head")) * size, size)
        brought = pltpu.make_async_copy(w_ref.at[:, pl.ds(start, size)], w_out, sem)
        brought.start()
    elif last:
        att_refs = refs[:2]
        m_ref, o_ref = refs[2:4]
        refs = refs[4:]
    else:
        m_ref, o_ref = refs[:2]
        refs = refs[2:]
    kv_ref, qt_ref, flag_ref, x_ref, tag_ref, lo_ref, hi_ref = refs[:7]
    p_refs, lists = refs[7:9], refs[9:15]
    k0_ref, k1_ref, v0_ref, v1_ref, which_ref, col_ref = lists

    places = [(p, i * ROWS) for p, count in zip(pieces, counts) for i in range(count)]
    total = len(places)
    for i, (piece, base) in enumerate(places):
        tag_ref[i] = tag_of(piece, base)
        for half in range(2):
            kv_ref[2 * i + half] = piece[base + half * BLK : base + half * BLK + BLK, :]
    kv_ref[2 * total] = jnp.zeros((BLK, 2 * HD), jnp.bfloat16)
    lane = lax.broadcasted_iota(jnp.int32, (16, 2 * BLK), 1)
    for i, most in enumerate((2 * BLK, BLK, 0)):
        flag_ref[i] = jnp.where(lane < most, 1.0, 0.0).astype(jnp.bfloat16)

    qt_ref[...] = q_in[...]
    list_steps(total, tag_ref, b_ref, lo_ref, hi_ref, lists)
    m_ref[...] = m_base[...]
    o_ref[...] = o_base[...]
    x_ref[...] = jnp.full(x_ref.shape, LOWEST, jnp.float32)

    def keys(step):
        return jnp.concatenate([kv_ref[k0_ref[step], :, :HD], kv_ref[k1_ref[step], :, :HD]], axis=0)

    def values(step):
        return jnp.concatenate([kv_ref[v0_ref[step], :, HD:], kv_ref[v1_ref[step], :, HD:]], axis=0)

    def weigh(step, slot):
        k = keys(step)
        for c in range(0, QW, TILE):
            cols = columns(col_ref[step] + c, TILE)
            scores = jnp.dot(k, qt_ref[:, cols], preferred_element_type=jnp.float32)
            p_refs[slot][:, c : c + TILE] = jnp.exp2(scores * SCALE - m_ref[:, cols]).astype(
                jnp.bfloat16
            )
            x_ref[:, cols] = jnp.maximum(
                x_ref[:, cols], jnp.max(scores.reshape(2 * BLK // 8, 8, TILE), axis=0)
            )

    def add(step, slot):
        terms = jnp.concatenate([values(step).T, flag_ref[which_ref[step]]], axis=0)
        for c in range(0, QW, TILE):
            cols = columns(col_ref[step] + c, TILE)
            o_ref[:, cols] += jnp.dot(
                terms, p_refs[slot][:, c : c + TILE], preferred_element_type=jnp.float32
            )[:SUMS]

    steps = 2 * total + 2

    def turn(j, carry):
        for i in range(UNROLL):
            weigh(UNROLL * j + 1 + i, 1 - i % 2)
            add(UNROLL * j + i, i % 2)
        return carry

    turns = (steps - 1) // UNROLL
    weigh(0, 0)
    lax.fori_loop(0, turns, turn, 0)
    for i in range(UNROLL * turns, steps):
        if i + 1 < steps:
            weigh(i + 1, 1 - i % 2)
        add(i, i % 2)

    @pl.when(jnp.max(x_ref[...] * SCALE - m_ref[...]) > HEADROOM)
    def _():
        m_ref[...] = m_base[...]
        o_ref[...] = o_base[...]

        def again(step, carry):
            cols = columns(col_ref[step], QW)
            scores = jnp.dot(keys(step), qt_ref[:, cols], preferred_element_type=jnp.float32)
            fold(scores, values(step), flag_ref[which_ref[step]], cols, m_ref, o_ref)
            return carry

        lax.fori_loop(0, steps, again, 0)

    if fetch:
        brought.wait()

    if last:
        for s in range(2):
            for half in range(2):
                start = ((1 - half) * 2 + s) * QW
                cols = slice(start, start + QW)
                done = (o_ref[:HD, cols] / o_ref[HD : HD + 1, cols]).T
                for h in range(GROUP):
                    att_refs[s][half * BLK : (half + 1) * BLK, h * HD : (h + 1) * HD] = done[
                        h * BLK : (h + 1) * BLK
                    ].astype(jnp.bfloat16)


def attend(pieces, state, last=False, weight=None):
    counts = tuple(p.shape[0] // ROWS for p in pieces)
    total = sum(counts)
    vmem = pl.BlockSpec(memory_space=pltpu.VMEM)
    smem = pl.BlockSpec(memory_space=pltpu.SMEM)
    width = 4 * QW
    kept = [(1, width), (SUMS, width)]
    if last:
        outs = [jax.ShapeDtypeStruct((2 * BLK, GROUP * HD), jnp.bfloat16)] * 2
        scratch = [pltpu.VMEM(shape, jnp.float32) for shape in kept]
    else:
        outs = [jax.ShapeDtypeStruct(shape, jnp.float32) for shape in kept]
        scratch = []
    in_specs = [vmem] * len(pieces) + [smem] + [vmem] * 3
    fetch = weight is not None
    more = []
    if fetch:
        in_specs.append(pl.BlockSpec(memory_space=pltpu.HBM))
        outs.append(
            jax.ShapeDtypeStruct((weight.shape[0], weight.shape[1] // 2), weight.dtype)
        )
        state = [*state, weight]
        more = [pltpu.SemaphoreType.DMA]
    cells = total * 2 * BLK * BLK * 2 * GROUP
    return pl.pallas_call(
        functools.partial(attend_kernel, counts, last, fetch),
        out_shape=outs,
        in_specs=in_specs,
        out_specs=[vmem] * len(outs),
        scratch_shapes=scratch
        + [
            pltpu.VMEM((2 * total + 1, BLK, 2 * HD), jnp.bfloat16),
            pltpu.VMEM((HD, width), jnp.bfloat16),
            pltpu.VMEM((3, 16, 2 * BLK), jnp.bfloat16),
            pltpu.VMEM((8, width), jnp.float32),
        ]
        + [pltpu.SMEM((total + 1,), jnp.int32)] * 3
        + [pltpu.VMEM((2 * BLK, QW), jnp.bfloat16)] * 2
        + [pltpu.SMEM((2 * total + 2,), jnp.int32)] * 6
        + more,
        cost_estimate=pl.CostEstimate(
            flops=4 * HD * cells, transcendentals=cells, bytes_accessed=total * ROWS * 512
        ),
        compiler_params=pltpu.CompilerParams(
            vmem_limit_bytes=FETCH_VMEM_BYTES if fetch else VMEM_BYTES
        ),
    )(*pieces, *state)


def join_kernel(number, *refs):
    parts, whole, sems = refs[:number], refs[number], refs[number + 1]
    copies, at = [], 0
    for i, part in enumerate(parts):
        rows = part.shape[0]
        copies.append(pltpu.make_async_copy(part, whole.at[pl.ds(at, rows)], sems.at[i]))
        at += rows
    for copy in copies:
        copy.start()
    for copy in copies:
        copy.wait()


def joined(parts):
    rows = sum(p.shape[0] for p in parts)
    anywhere = pl.BlockSpec(memory_space=pl.ANY)
    return pl.pallas_call(
        functools.partial(join_kernel, len(parts)),
        out_shape=jax.ShapeDtypeStruct((rows, parts[0].shape[1]), parts[0].dtype),
        in_specs=[anywhere] * len(parts),
        out_specs=anywhere,
        scratch_shapes=[pltpu.SemaphoreType.DMA((len(parts),))],
        compiler_params=pltpu.CompilerParams(vmem_limit_bytes=VMEM_BYTES),
    )(*parts)


def near(array, axis):
    return [shifted(array, axis, 1), shifted(array, axis, -1)]


def far(pair, axis):
    half = pair[0].shape[0] // 2
    return [shifted(pair[0][:half], axis, 1), shifted(pair[1][half:], axis, -1)]


def after(pairs, token):
    *arrays, _ = lax.optimization_barrier((*sum(pairs, []), token))
    return [arrays[i : i + 2] for i in range(0, len(arrays), 2)]


def project_kernel(others, theirs, start, size, with_sum, *refs):
    number = len(others)
    att_refs, w_ref = refs[:number], refs[number]
    w_buf, sems = refs[-2:]
    out_ref = refs[-3]
    core, head = lax.axis_index("core"), lax.axis_index("head")
    rows = w_ref.shape[0] // 2
    half = w_ref.shape[1] // 2
    side = 1 - head if theirs else head
    blocks = size // WCOLS
    copies = []
    for j in range(blocks):
        for i, other in enumerate(others):
            row = (1 - core if other else core) * rows
            col = side * half + start + j * WCOLS
            at = j * number + i
            copies.append(
                pltpu.make_async_copy(
                    w_ref.at[
                        pl.ds(pl.multiple_of(row, rows), rows),
                        pl.ds(pl.multiple_of(col, WCOLS), WCOLS),
                    ],
                    w_buf.at[at],
                    sems.at[at],
                )
            )
    for copy in copies:
        copy.start()
    for j in range(blocks):
        cols = slice(j * WCOLS, (j + 1) * WCOLS)
        total = refs[number + 1][:, start + j * WCOLS : start + (j + 1) * WCOLS] if with_sum else 0.0
        for i, att_ref in enumerate(att_refs):
            copies[j * number + i].wait()
            total = total + jnp.dot(
                att_ref[...], w_buf[j * number + i], preferred_element_type=jnp.float32
            )
        out_ref[:, cols] = total.astype(out_ref.dtype)


def project(atts, others, weight, theirs, start, size, dtype, total=None):
    vmem = pl.BlockSpec(memory_space=pltpu.VMEM)
    rows, width = atts[0].shape
    pieces = len(atts) * size // WCOLS
    sums = [] if total is None else [total]
    return pl.pallas_call(
        functools.partial(project_kernel, others, theirs, start, size, total is not None),
        in_specs=[vmem] * len(atts) + [pl.BlockSpec(memory_space=pltpu.HBM)] + [vmem] * len(sums),
        out_specs=vmem,
        out_shape=jax.ShapeDtypeStruct((rows, size), dtype),
        scratch_shapes=[
            pltpu.VMEM((pieces, width, WCOLS), jnp.bfloat16),
            pltpu.SemaphoreType.DMA((pieces,)),
        ],
        cost_estimate=pl.CostEstimate(
            flops=2 * rows * width * len(atts) * size,
            transcendentals=0,
            bytes_accessed=2 * width * len(atts) * size,
        ),
        compiler_params=pltpu.CompilerParams(vmem_limit_bytes=KEEP_VMEM_BYTES),
    )(*atts, weight, *sums)


def send_kernel(other, start, with_sum, att_ref, w_ref, *refs):
    out_ref = refs[-1]
    core = lax.axis_index("core")
    rows = w_ref.shape[0] // 2
    row = pl.multiple_of((1 - core if other else core) * rows, rows)
    cols = slice(start, start + out_ref.shape[1])
    total = jnp.dot(
        att_ref[...], w_ref[pl.ds(row, rows), cols], preferred_element_type=jnp.float32
    )
    if with_sum:
        total = total + refs[0][:, cols]
    out_ref[...] = total.astype(out_ref.dtype)


def send_part(att, weight, other, start, size, dtype, sums=()):
    vmem = pl.BlockSpec(memory_space=pltpu.VMEM)
    rows, width = att.shape
    return pl.pallas_call(
        functools.partial(send_kernel, other, start, len(sums) > 0),
        in_specs=[vmem] * (2 + len(sums)),
        out_specs=vmem,
        out_shape=jax.ShapeDtypeStruct((rows, size), dtype),
        cost_estimate=pl.CostEstimate(
            flops=2 * rows * width * size, transcendentals=0, bytes_accessed=2 * width * size
        ),
        compiler_params=pltpu.CompilerParams(vmem_limit_bytes=VMEM_BYTES),
    )(att, weight, *sums)


def shards(queries, key_states, value_states, positions, out_weight):
    first_core = lax.axis_index("core") == 0
    tag = lax.div(positions[0], BLK).astype(jnp.bfloat16)

    def packed(low):
        parts = [jnp.where(low, a[:, :HD], a[:, HD:]) for a in (key_states, value_states)]
        return jnp.pad(
            jnp.concatenate(parts, axis=1), ((0, ROWS - 2 * BLK), (0, 0)), constant_values=tag
        )

    given = shifted(packed(~first_core), "core", 1)
    both = joined([packed(first_core), given])
    whole, _ = lax.optimization_barrier((queries, both))
    width = GROUP * HD
    q_given = shifted(jnp.where(first_core, whole[:, width:], whole[:, :width]), "core", 1)

    beyond = shifted(both, "z", 1)
    near_a = near(both, "x")
    b_both, qt, *state = begin(both, queries, q_given)
    near_b = near(beyond, "y")
    far_a, far_b = far(near_a, "x"), far(near_b, "y")
    all_a = joined([both] + near_a + far_a)
    all_b = joined([beyond] + near_b + far_b)
    near_a, near_b = near(all_a, "y"), near(all_b, "x")
    *state, w_send = attend([all_a, all_b], [b_both, qt, *state], weight=out_weight)
    near_a, near_b = after([near_a, near_b], state[0])
    far_a, far_b = far(near_a, "y"), far(near_b, "x")
    state = attend(near_a + near_b, [b_both, qt, *state])
    mine, returned = attend(far_a + far_b, [b_both, qt, *state], last=True)[:2]

    returned = shifted(returned, "core", 1)
    half = out_weight.shape[1] // 2
    sums = send_part(mine, w_send, False, 0, half, jnp.float32)
    swapped = shifted(
        send_part(returned, w_send, True, 0, half, jnp.bfloat16, [sums]), "head", 1
    )
    kept = project([mine, returned], [False, True], out_weight, False, 0, half, jnp.float32)
    return (kept + swapped.astype(jnp.float32)).astype(jnp.bfloat16)


def solution(mesh):
    split = Mesh(mesh.devices.reshape(2, 4, 4, 2, 2), ("z", "y", "x", "core", "head"))
    seq = ("z", "y", "x", "core")
    in_specs = (P(seq, "head"), P(seq, "head"), P(seq, "head"), P(seq), P("head", None))
    return jax.shard_map(
        shards, mesh=split, in_specs=in_specs, out_specs=P(seq, "head"), check_vma=False
    )
```

```python
import functools

import jax
import jax.numpy as jnp
import numpy as np
from jax import lax
from jax.experimental import pallas as pl
from jax.experimental.pallas import tpu as pltpu
from jax.sharding import Mesh, PartitionSpec as P

HD = 128
GROUP = 8
BLK = 96
ROWS = 200
QW = GROUP * BLK
SCALE = 1.4426950408889634 * HD**-0.5
LOWEST = -1e30
VMEM_BYTES = 24 << 20
FETCH_VMEM_BYTES = 30 << 20
KEEP_VMEM_BYTES = 48 << 20
TILE = 768
SUMS = HD + 8
HEADROOM = 60.0
UNROLL = 8
WCOLS = 512


def shifted(array, axis, by):
    size = lax.axis_size(axis)
    return lax.ppermute(array, axis, [(i, (i + by) % size) for i in range(size)])


def columns(start, size):
    return pl.ds(pl.multiple_of(start, HD), size)


def fold(scores, values, flags, cols, m_ref, o_ref):
    old = m_ref[:, cols]
    new = jnp.maximum(old, jnp.max(scores, axis=0, keepdims=True) * SCALE)
    weights = jnp.exp2(scores * SCALE - new).astype(jnp.bfloat16)
    m_ref[:, cols] = new
    terms = jnp.concatenate([values.T, flags], axis=0)
    o_ref[:, cols] = (
        o_ref[:, cols] * jnp.exp2(old - new)
        + jnp.dot(terms, weights, preferred_element_type=jnp.float32)[:SUMS]
    )


def list_steps(total, tag_ref, b_ref, lo_ref, hi_ref, lists):
    def write(step, *entries):
        for ref, entry in zip(lists, entries):
            ref[step] = jnp.asarray(entry, jnp.int32)

    half = total // 2
    for s in range(2):
        for p in range(half):
            write(s * half + p, 4 * p, 4 * p + 2, 4 * p, 4 * p + 2, 0, s * QW)
    for s in range(2):
        low_count = high_count = jnp.int32(0)
        for d in range(total):
            low = jnp.where(tag_ref[d] < b_ref[s], 1, 0).astype(jnp.int32)
            high = jnp.where(tag_ref[d] > b_ref[s], 1, 0).astype(jnp.int32)
            lo_ref[low_count] = jnp.int32(2 * d)
            hi_ref[high_count] = jnp.int32(2 * d + 1)
            low_count = low_count + low
            high_count = high_count + high
        low_steps = lax.div(low_count + 1, 2)

        def build(t, carry, s=s, low_count=low_count, high_count=high_count, low_steps=low_steps):
            is_low = t < low_steps
            u = 2 * jnp.where(is_low, t, t - low_steps)
            count = jnp.where(is_low, low_count, high_count)
            u0, u1 = jnp.minimum(u, total - 1), jnp.minimum(u + 1, total - 1)
            there, paired = u < count, u + 1 < count
            a0 = jnp.where(there, jnp.where(is_low, lo_ref[u0], hi_ref[u0]), 0)
            a1 = jnp.where(paired, jnp.where(is_low, lo_ref[u1], hi_ref[u1]), a0)
            nothing = 2 * total
            write(
                total + s * (half + 1) + t,
                a0,
                a1,
                jnp.where(there, a0, nothing),
                jnp.where(paired, a1, nothing),
                jnp.where(there, jnp.where(paired, 0, 1), 2),
                jnp.where(is_low, 2 * QW, 0) + s * QW,
            )
            return carry

        lax.fori_loop(0, half + 1, build, 0)


def tag_of(piece, base):
    rows = piece[base + 2 * BLK : base + 2 * BLK + 8, :HD]
    return jnp.max(rows.astype(jnp.float32)).astype(jnp.int32)


def begin_kernel(both_ref, whole_ref, q_given, b_ref, qt_ref, m_ref, o_ref, q_own, flag_ref, sem):
    width = GROUP * HD
    mine = pl.ds(pl.multiple_of(lax.axis_index("core") * width, HD), width)
    fetch = pltpu.make_async_copy(whole_ref.at[:, mine], q_own, sem)
    fetch.start()
    m_ref[...] = jnp.full(m_ref.shape, LOWEST, jnp.float32)
    o_ref[...] = jnp.zeros(o_ref.shape, jnp.float32)
    flag_ref[...] = jnp.ones(flag_ref.shape, jnp.bfloat16)
    token = lax.rem(lax.broadcasted_iota(jnp.int32, (1, QW), 1), BLK)
    seen = lax.broadcasted_iota(jnp.int32, (BLK, QW), 0) <= token
    fetch.wait()
    for s in range(2):
        base = s * ROWS
        b_ref[s] = tag_of(both_ref, base)
        for half in range(2):
            rows = slice(half * BLK, half * BLK + BLK)
            q_ref = (q_own, q_given)[s]
            tall = jnp.concatenate([q_ref[rows, h * HD : (h + 1) * HD] for h in range(GROUP)], axis=0)
            start = ((1 - half) * 2 + s) * QW
            cols = slice(start, start + QW)
            qt_ref[:, cols] = tall.T
            block = both_ref[base + half * BLK : base + half * BLK + BLK, :]
            scores = jnp.dot(block[:, :HD], qt_ref[:, cols], preferred_element_type=jnp.float32)
            scores = jnp.where(seen, scores, LOWEST)
            fold(scores, block[:, HD:], flag_ref[...], cols, m_ref, o_ref)


def begin(both, queries, q_given):
    vmem = pl.BlockSpec(memory_space=pltpu.VMEM)
    width = 4 * QW
    return pl.pallas_call(
        begin_kernel,
        out_shape=[
            jax.ShapeDtypeStruct((2,), jnp.int32),
            jax.ShapeDtypeStruct((HD, width), jnp.bfloat16),
            jax.ShapeDtypeStruct((1, width), jnp.float32),
            jax.ShapeDtypeStruct((SUMS, width), jnp.float32),
        ],
        in_specs=[vmem, pl.BlockSpec(memory_space=pltpu.HBM), vmem],
        out_specs=[pl.BlockSpec(memory_space=pltpu.SMEM)] + [vmem] * 3,
        scratch_shapes=[
            pltpu.VMEM((2 * BLK, GROUP * HD), jnp.bfloat16),
            pltpu.VMEM((16, BLK), jnp.bfloat16),
            pltpu.SemaphoreType.DMA,
        ],
        cost_estimate=pl.CostEstimate(
            flops=16 * HD * BLK * QW, transcendentals=4 * BLK * QW, bytes_accessed=1 << 20
        ),
        compiler_params=pltpu.CompilerParams(vmem_limit_bytes=VMEM_BYTES),
    )(both, queries, q_given)


def attend_kernel(counts, last, fetch, *refs):
    number = len(counts)
    pieces = refs[:number]
    refs = refs[number:]
    b_ref, q_in, m_base, o_base = refs[:4]
    refs = refs[4:]
    if fetch:
        w_ref, m_ref, o_ref, w_out = refs[:4]
        refs, sem = refs[4:-1], refs[-1]
        size = w_out.shape[1]
        start = pl.multiple_of((1 - lax.axis_index("head")) * size, size)
        brought = pltpu.make_async_copy(w_ref.at[:, pl.ds(start, size)], w_out, sem)
        brought.start()
    elif last:
        att_refs = refs[:2]
        m_ref, o_ref = refs[2:4]
        refs = refs[4:]
    else:
        m_ref, o_ref = refs[:2]
        refs = refs[2:]
    kv_ref, qt_ref, flag_ref, x_ref, tag_ref, lo_ref, hi_ref = refs[:7]
    p_refs, lists = refs[7:9], refs[9:15]
    k0_ref, k1_ref, v0_ref, v1_ref, which_ref, col_ref = lists

    places = [(p, i * ROWS) for p, count in zip(pieces, counts) for i in range(count)]
    total = len(places)
    for i, (piece, base) in enumerate(places):
        tag_ref[i] = tag_of(piece, base)
        for half in range(2):
            kv_ref[2 * i + half] = piece[base + half * BLK : base + half * BLK + BLK, :]
    kv_ref[2 * total] = jnp.zeros((BLK, 2 * HD), jnp.bfloat16)
    lane = lax.broadcasted_iota(jnp.int32, (16, 2 * BLK), 1)
    for i, most in enumerate((2 * BLK, BLK, 0)):
        flag_ref[i] = jnp.where(lane < most, 1.0, 0.0).astype(jnp.bfloat16)

    qt_ref[...] = q_in[...]
    list_steps(total, tag_ref, b_ref, lo_ref, hi_ref, lists)
    m_ref[...] = m_base[...]
    o_ref[...] = o_base[...]
    x_ref[...] = jnp.full(x_ref.shape, LOWEST, jnp.float32)

    def keys(step):
        return jnp.concatenate([kv_ref[k0_ref[step], :, :HD], kv_ref[k1_ref[step], :, :HD]], axis=0)

    def values(step):
        return jnp.concatenate([kv_ref[v0_ref[step], :, HD:], kv_ref[v1_ref[step], :, HD:]], axis=0)

    def weigh(step, slot):
        k = keys(step)
        for c in range(0, QW, TILE):
            cols = columns(col_ref[step] + c, TILE)
            scores = jnp.dot(k, qt_ref[:, cols], preferred_element_type=jnp.float32)
            p_refs[slot][:, c : c + TILE] = jnp.exp2(scores * SCALE - m_ref[:, cols]).astype(
                jnp.bfloat16
            )
            x_ref[:, cols] = jnp.maximum(
                x_ref[:, cols], jnp.max(scores.reshape(2 * BLK // 8, 8, TILE), axis=0)
            )

    def add(step, slot):
        terms = jnp.concatenate([values(step).T, flag_ref[which_ref[step]]], axis=0)
        for c in range(0, QW, TILE):
            cols = columns(col_ref[step] + c, TILE)
            o_ref[:, cols] += jnp.dot(
                terms, p_refs[slot][:, c : c + TILE], preferred_element_type=jnp.float32
            )[:SUMS]

    steps = 2 * total + 2

    def turn(j, carry):
        for i in range(UNROLL):
            weigh(UNROLL * j + 1 + i, 1 - i % 2)
            add(UNROLL * j + i, i % 2)
        return carry

    turns = (steps - 1) // UNROLL
    weigh(0, 0)
    lax.fori_loop(0, turns, turn, 0)
    for i in range(UNROLL * turns, steps):
        if i + 1 < steps:
            weigh(i + 1, 1 - i % 2)
        add(i, i % 2)

    @pl.when(jnp.max(x_ref[...] * SCALE - m_ref[...]) > HEADROOM)
    def _():
        m_ref[...] = m_base[...]
        o_ref[...] = o_base[...]

        def again(step, carry):
            cols = columns(col_ref[step], QW)
            scores = jnp.dot(keys(step), qt_ref[:, cols], preferred_element_type=jnp.float32)
            fold(scores, values(step), flag_ref[which_ref[step]], cols, m_ref, o_ref)
            return carry

        lax.fori_loop(0, steps, again, 0)

    if fetch:
        brought.wait()

    if last:
        for s in range(2):
            for half in range(2):
                start = ((1 - half) * 2 + s) * QW
                cols = slice(start, start + QW)
                done = (o_ref[:HD, cols] / o_ref[HD : HD + 1, cols]).T
                for h in range(GROUP):
                    att_refs[s][half * BLK : (half + 1) * BLK, h * HD : (h + 1) * HD] = done[
                        h * BLK : (h + 1) * BLK
                    ].astype(jnp.bfloat16)


def attend(pieces, state, last=False, weight=None):
    counts = tuple(p.shape[0] // ROWS for p in pieces)
    total = sum(counts)
    vmem = pl.BlockSpec(memory_space=pltpu.VMEM)
    smem = pl.BlockSpec(memory_space=pltpu.SMEM)
    width = 4 * QW
    kept = [(1, width), (SUMS, width)]
    if last:
        outs = [jax.ShapeDtypeStruct((2 * BLK, GROUP * HD), jnp.bfloat16)] * 2
        scratch = [pltpu.VMEM(shape, jnp.float32) for shape in kept]
    else:
        outs = [jax.ShapeDtypeStruct(shape, jnp.float32) for shape in kept]
        scratch = []
    in_specs = [vmem] * len(pieces) + [smem] + [vmem] * 3
    fetch = weight is not None
    more = []
    if fetch:
        in_specs.append(pl.BlockSpec(memory_space=pltpu.HBM))
        outs.append(
            jax.ShapeDtypeStruct((weight.shape[0], weight.shape[1] // 2), weight.dtype)
        )
        state = [*state, weight]
        more = [pltpu.SemaphoreType.DMA]
    cells = total * 2 * BLK * BLK * 2 * GROUP
    return pl.pallas_call(
        functools.partial(attend_kernel, counts, last, fetch),
        out_shape=outs,
        in_specs=in_specs,
        out_specs=[vmem] * len(outs),
        scratch_shapes=scratch
        + [
            pltpu.VMEM((2 * total + 1, BLK, 2 * HD), jnp.bfloat16),
            pltpu.VMEM((HD, width), jnp.bfloat16),
            pltpu.VMEM((3, 16, 2 * BLK), jnp.bfloat16),
            pltpu.VMEM((8, width), jnp.float32),
        ]
        + [pltpu.SMEM((total + 1,), jnp.int32)] * 3
        + [pltpu.VMEM((2 * BLK, QW), jnp.bfloat16)] * 2
        + [pltpu.SMEM((2 * total + 2,), jnp.int32)] * 6
        + more,
        cost_estimate=pl.CostEstimate(
            flops=4 * HD * cells, transcendentals=cells, bytes_accessed=total * ROWS * 512
        ),
        compiler_params=pltpu.CompilerParams(
            vmem_limit_bytes=FETCH_VMEM_BYTES if fetch else VMEM_BYTES
        ),
    )(*pieces, *state)


def join_kernel(number, *refs):
    parts, whole, sems = refs[:number], refs[number], refs[number + 1]
    copies, at = [], 0
    for i, part in enumerate(parts):
        rows = part.shape[0]
        copies.append(pltpu.make_async_copy(part, whole.at[pl.ds(at, rows)], sems.at[i]))
        at += rows
    for copy in copies:
        copy.start()
    for copy in copies:
        copy.wait()


def joined(parts):
    rows = sum(p.shape[0] for p in parts)
    anywhere = pl.BlockSpec(memory_space=pl.ANY)
    return pl.pallas_call(
        functools.partial(join_kernel, len(parts)),
        out_shape=jax.ShapeDtypeStruct((rows, parts[0].shape[1]), parts[0].dtype),
        in_specs=[anywhere] * len(parts),
        out_specs=anywhere,
        scratch_shapes=[pltpu.SemaphoreType.DMA((len(parts),))],
        compiler_params=pltpu.CompilerParams(vmem_limit_bytes=VMEM_BYTES),
    )(*parts)


def near(array, axis):
    return [shifted(array, axis, 1), shifted(array, axis, -1)]


def far(pair, axis):
    half = pair[0].shape[0] // 2
    return [shifted(pair[0][:half], axis, 1), shifted(pair[1][half:], axis, -1)]


def after(pairs, token):
    *arrays, _ = lax.optimization_barrier((*sum(pairs, []), token))
    return [arrays[i : i + 2] for i in range(0, len(arrays), 2)]


def project_kernel(others, theirs, start, size, with_sum, *refs):
    number = len(others)
    att_refs, w_ref = refs[:number], refs[number]
    w_buf, sems = refs[-2:]
    out_ref = refs[-3]
    core, head = lax.axis_index("core"), lax.axis_index("head")
    rows = w_ref.shape[0] // 2
    half = w_ref.shape[1] // 2
    side = 1 - head if theirs else head
    blocks = size // WCOLS
    copies = []
    for j in range(blocks):
        for i, other in enumerate(others):
            row = (1 - core if other else core) * rows
            col = side * half + start + j * WCOLS
            at = j * number + i
            copies.append(
                pltpu.make_async_copy(
                    w_ref.at[
                        pl.ds(pl.multiple_of(row, rows), rows),
                        pl.ds(pl.multiple_of(col, WCOLS), WCOLS),
                    ],
                    w_buf.at[at],
                    sems.at[at],
                )
            )
    for copy in copies:
        copy.start()
    for j in range(blocks):
        cols = slice(j * WCOLS, (j + 1) * WCOLS)
        total = refs[number + 1][:, start + j * WCOLS : start + (j + 1) * WCOLS] if with_sum else 0.0
        for i, att_ref in enumerate(att_refs):
            copies[j * number + i].wait()
            total = total + jnp.dot(
                att_ref[...], w_buf[j * number + i], preferred_element_type=jnp.float32
            )
        out_ref[:, cols] = total.astype(out_ref.dtype)


def project(atts, others, weight, theirs, start, size, dtype, total=None):
    vmem = pl.BlockSpec(memory_space=pltpu.VMEM)
    rows, width = atts[0].shape
    pieces = len(atts) * size // WCOLS
    sums = [] if total is None else [total]
    return pl.pallas_call(
        functools.partial(project_kernel, others, theirs, start, size, total is not None),
        in_specs=[vmem] * len(atts) + [pl.BlockSpec(memory_space=pltpu.HBM)] + [vmem] * len(sums),
        out_specs=vmem,
        out_shape=jax.ShapeDtypeStruct((rows, size), dtype),
        scratch_shapes=[
            pltpu.VMEM((pieces, width, WCOLS), jnp.bfloat16),
            pltpu.SemaphoreType.DMA((pieces,)),
        ],
        cost_estimate=pl.CostEstimate(
            flops=2 * rows * width * len(atts) * size,
            transcendentals=0,
            bytes_accessed=2 * width * len(atts) * size,
        ),
        compiler_params=pltpu.CompilerParams(vmem_limit_bytes=KEEP_VMEM_BYTES),
    )(*atts, weight, *sums)


def send_kernel(other, start, with_sum, att_ref, w_ref, *refs):
    out_ref = refs[-1]
    core = lax.axis_index("core")
    rows = w_ref.shape[0] // 2
    row = pl.multiple_of((1 - core if other else core) * rows, rows)
    cols = slice(start, start + out_ref.shape[1])
    total = jnp.dot(
        att_ref[...], w_ref[pl.ds(row, rows), cols], preferred_element_type=jnp.float32
    )
    if with_sum:
        total = total + refs[0][:, cols]
    out_ref[...] = total.astype(out_ref.dtype)


def send_part(att, weight, other, start, size, dtype, sums=()):
    vmem = pl.BlockSpec(memory_space=pltpu.VMEM)
    rows, width = att.shape
    return pl.pallas_call(
        functools.partial(send_kernel, other, start, len(sums) > 0),
        in_specs=[vmem] * (2 + len(sums)),
        out_specs=vmem,
        out_shape=jax.ShapeDtypeStruct((rows, size), dtype),
        cost_estimate=pl.CostEstimate(
            flops=2 * rows * width * size, transcendentals=0, bytes_accessed=2 * width * size
        ),
        compiler_params=pltpu.CompilerParams(vmem_limit_bytes=VMEM_BYTES),
    )(att, weight, *sums)


def shards(queries, key_states, value_states, positions, out_weight):
    first_core = lax.axis_index("core") == 0
    tag = lax.div(positions[0], BLK).astype(jnp.bfloat16)

    def packed(low):
        parts = [jnp.where(low, a[:, :HD], a[:, HD:]) for a in (key_states, value_states)]
        return jnp.pad(
            jnp.concatenate(parts, axis=1), ((0, ROWS - 2 * BLK), (0, 0)), constant_values=tag
        )

    given = shifted(packed(~first_core), "core", 1)
    both = joined([packed(first_core), given])
    whole, _ = lax.optimization_barrier((queries, both))
    width = GROUP * HD
    q_given = shifted(jnp.where(first_core, whole[:, width:], whole[:, :width]), "core", 1)

    beyond = shifted(both, "z", 1)
    near_a = near(both, "x")
    b_both, qt, *state = begin(both, queries, q_given)
    near_b = near(beyond, "y")
    far_a, far_b = far(near_a, "x"), far(near_b, "y")
    far_a, far_b = after([far_a, far_b], state[0])
    all_a = joined([both] + near_a + far_a)
    all_b = joined([beyond] + near_b + far_b)
    near_a, near_b = near(all_a, "y"), near(all_b, "x")
    *state, w_send = attend([all_a, all_b], [b_both, qt, *state], weight=out_weight)
    (near_a,) = after([near_a], state[0])
    far_a = far(near_a, "y")
    state = attend(near_a, [b_both, qt, *state])
    (near_b,) = after([near_b], state[0])
    far_b = far(near_b, "x")
    state = attend(near_b + far_a, [b_both, qt, *state])
    mine, returned = attend(far_b, [b_both, qt, *state], last=True)

    returned = shifted(returned, "core", 1)
    half = out_weight.shape[1] // 2
    sums = send_part(mine, w_send, False, 0, half, jnp.float32)
    swapped = shifted(
        send_part(returned, w_send, True, 0, half, jnp.bfloat16, [sums]), "head", 1
    )
    kept = project([mine, returned], [False, True], out_weight, False, 0, half, jnp.float32)
    return (kept + swapped.astype(jnp.float32)).astype(jnp.bfloat16)


def solution(mesh):
    split = Mesh(mesh.devices.reshape(2, 4, 4, 2, 2), ("z", "y", "x", "core", "head"))
    seq = ("z", "y", "x", "core")
    in_specs = (P(seq, "head"), P(seq, "head"), P(seq, "head"), P(seq), P("head", None))
    return jax.shard_map(
        shards, mesh=split, in_specs=in_specs, out_specs=P(seq, "head"), check_vma=False
    )
```
